64 devices in a mesh: rep: 4 (over x, y), dp: 16 (over z, core).
Axes of the slice: x: 2, y: 2, z: 8, core: 2. Of those that a mesh axis runs over, the one named last changes fastest.
The devices are a block of a 4x4x8 slice.
Arguments:
- x: bfloat16 [64, 1024, 768], P(('rep', 'dp')), parts along dimension 0
- dy: bfloat16 [64, 1024, 768], P(('rep', 'dp')), parts along dimension 0
- w_gate: bfloat16 [2, 768, 3072], replicated
- w_up: bfloat16 [2, 768, 3072], replicated
- w_down: bfloat16 [2, 3072, 768], replicated
- m_w_gate: float32 [2, 768, 3072], P(None, 'dp')
- m_w_up: float32 [2, 768, 3072], P(None, 'dp')
- m_w_down: float32 [2, 3072, 768], P(None, 'dp')
- v_w_gate: float32 [2, 768, 3072], P(None, 'dp')
- v_w_up: float32 [2, 768, 3072], P(None, 'dp')
- v_w_down: float32 [2, 3072, 768], P(None, 'dp')
Outputs:
- output 1: bfloat16 [8, 768, 3072], P('rep'), parts along dimension 0
- output 2: bfloat16 [8, 768, 3072], P('rep'), parts along dimension 0
- output 3: bfloat16 [8, 3072, 768], P('rep'), parts along dimension 0
- output 4: float32 [8, 768, 3072], P('rep', 'dp'), parts along dimension 0
- output 5: float32 [8, 768, 3072], P('rep', 'dp'), parts along dimension 0
- output 6: float32 [8, 3072, 768], P('rep', 'dp'), parts along dimension 0
- output 7: float32 [8, 768, 3072], P('rep', 'dp'), parts along dimension 0
- output 8: float32 [8, 768, 3072], P('rep', 'dp'), parts along dimension 0
- output 9: float32 [8, 3072, 768], P('rep', 'dp'), parts along dimension 0
There are 4 independent parts. The reference program is written for one: setup_inputs(seed, part) draws one part's arguments, and reference() takes and returns one part's arrays. A program takes and returns all parts, laid end to end along the dimension named above; an argument that names none is the same for every part.
All inputs are finite; a program needn't handle non-finite values.
Results may differ from the reference program's by a relative error of at most 0.022.
Values are sent between devices in bfloat16 or wider.
A program may use at most 768 MiB of HBM per device.

```python
import jax
import jax.numpy as jnp
from jax import lax

SEQUENCES = 16
TOKENS = 1024
D = 768
FF = 3072
LAYERS = 2
NAMES = ("w_gate", "w_up", "w_down")
SHAPES = {"w_gate": (LAYERS, D, FF), "w_up": (LAYERS, D, FF), "w_down": (LAYERS, FF, D)}


def bump(key, n, height):
    away = (jnp.arange(n, dtype=jnp.int32) - jax.random.randint(key, (), 0, n, jnp.int32)) % n
    return jnp.where(away < n // 8, height, 1.0)


def together(key, own, strength):
    shared = jax.random.normal(key, own.shape[1:], jnp.float32)
    return (own + strength * shared) * lax.rsqrt(1 + strength * strength)


def setup_inputs(seed: int = 0, part: int = 0) -> dict:
    kx, kdy, ka, kb, kz, kf, kh, kl, *keys = jax.random.split(jax.random.key(seed), 8 + 3 * len(NAMES))
    kx, kdy, ka, kb = (jax.random.fold_in(k, part) for k in (kx, kdy, ka, kb))
    kw, km, kv = (keys[i::3] for i in range(3))
    shape = (SEQUENCES, TOKENS, D)
    much_x, much_dy = jax.random.uniform(kz, (2,), jnp.float32, 0.0, 1.0)
    loud = 2.0 ** jax.random.uniform(jax.random.fold_in(kz, 1), (), jnp.float32, -1.0, 2.0)
    layers = 2.0 ** jax.random.uniform(kl, (LAYERS, 1, 1), jnp.float32, -1.0, 1.0)
    x = together(ka, jax.random.normal(kx, shape, jnp.float32), much_x) * bump(kf, D, 4.0)
    dy = together(kb, jax.random.normal(kdy, shape, jnp.float32), much_dy)
    drawn = {"x": x.astype(jnp.bfloat16), "dy": (loud * dy * (SEQUENCES * TOKENS) ** -0.5).astype(jnp.bfloat16)}
    for key, name in zip(kw, NAMES, strict=True):
        w = jax.random.normal(key, SHAPES[name], jnp.float32) * SHAPES[name][1] ** -0.5
        drawn[name] = (w * {"w_gate": 1.0, "w_up": bump(kh, FF, 4.0), "w_down": layers}[name]).astype(jnp.bfloat16)
    for key, name in zip(km, NAMES, strict=True):
        drawn[f"m_{name}"] = 0.1 * jax.random.normal(key, SHAPES[name], jnp.float32)
    for key, name in zip(kv, NAMES, strict=True):
        drawn[f"v_{name}"] = jax.random.uniform(key, SHAPES[name], jnp.float32, 0.005, 0.015)
    return drawn


def matmul(a, w):
    return jnp.dot(a, w, preferred_element_type=jnp.float32).astype(jnp.bfloat16)


def normed(h):
    wide = h.astype(jnp.float32)
    scale = lax.rsqrt(jnp.mean(wide**2, -1, keepdims=True) + 1e-6)
    return (wide * scale).astype(jnp.bfloat16)


def layer(h, w):
    a = normed(h)
    gate = jnp.dot(a, w["w_gate"], preferred_element_type=jnp.float32)
    up = jnp.dot(a, w["w_up"], preferred_element_type=jnp.float32)
    return h + matmul((jax.nn.silu(gate) * up).astype(jnp.bfloat16), w["w_down"])


def adamw(w, m, v, g):
    m = 0.9 * m + 0.1 * g
    v = 0.95 * v + 0.05 * g * g
    step = m * lax.rsqrt(v + 1e-8) + 0.1 * w
    return (w - 0.02 * step).astype(jnp.bfloat16), m, v


def clipped(gradients, sum_of_squares, count):
    factor = jnp.minimum(1.0, 0.5 * lax.rsqrt(sum_of_squares / count + 1e-30))
    return [g * factor for g in gradients]


def stack(weights, h):
    return lax.scan(lambda h, w: (layer(h, w), None), h, weights)[0]


def reference(x, dy, w_gate, w_up, w_down, m_w_gate, m_w_up, m_w_down, v_w_gate, v_w_up, v_w_down):
    weights = dict(zip(NAMES, (w_gate, w_up, w_down), strict=True))

    def take(so_far, sequence):
        h, by_y = sequence
        _, back = jax.vjp(lambda w: stack(w, h), weights)
        return jax.tree.map(lambda total, term: total + term.astype(jnp.float32), so_far, back(by_y)[0]), None

    none_yet = {name: jnp.zeros(w.shape, jnp.float32) for name, w in weights.items()}
    by_weights, _ = lax.scan(take, none_yet, (x, dy))
    gradients = [by_weights[name].astype(jnp.bfloat16).astype(jnp.float32) for name in NAMES]
    gradients = clipped(gradients, sum(jnp.sum(g * g) for g in gradients), sum(g.size for g in gradients))
    new = [
        adamw(w.astype(jnp.float32), m, v, g)
        for w, m, v, g in zip((w_gate, w_up, w_down), (m_w_gate, m_w_up, m_w_down), (v_w_gate, v_w_up, v_w_down), gradients, strict=True)
    ]
    return tuple(one[which] for which in range(3) for one in new)
```

```python
import functools

import jax
import jax.numpy as jnp
from jax import lax
from jax.experimental import pallas as pl
from jax.experimental.pallas import tpu as pltpu
from jax.sharding import PartitionSpec as P

F32, BF16 = jnp.float32, jnp.bfloat16
ANY, VMEM = pl.ANY, pltpu.VMEM
MESH = pl.DeviceIdType.MESH
VMEM_BYTES = 64 * 1024 * 1024 - 65536


def remote(src, dst, send, recv, to):
    return pltpu.make_async_remote_copy(
        src_ref=src, dst_ref=dst, send_sem=send, recv_sem=recv, device_id={"dp": to}, device_id_type=MESH
    )


def enter(peers):
    barrier = pltpu.get_barrier_semaphore()
    for peer in peers:
        pl.semaphore_signal(barrier, inc=1, device_id={"dp": peer}, device_id_type=MESH)
    pl.semaphore_wait(barrier, len(peers))


def sum_kernel(n, sources, *refs):
    inputs = refs[: len(sources)]
    g_ref, total_ref = refs[len(sources) : len(sources) + 2]
    (a_buf, b_buf, mine, theirs, ring, squares, slots, load_sem, swap_send, swap_recv, ring_send, ring_recv, all_send, all_recv) = refs[
        len(sources) + 2 :
    ]
    d = a_buf.shape[2]
    r, ff = mine.shape[2:]
    half, tiles, chips = ff // 2, ff // d, n // 2
    count = ring.shape[0]
    pairs = count // 2
    me = lax.axis_index("dp")
    z, c = lax.div(me, 2), lax.rem(me, 2)
    partner = 2 * z + 1 - c
    right = 2 * lax.rem(z + 1, chips) + c
    left = 2 * lax.rem(z + chips - 1, chips) + c
    onward = (right, left)

    def loads(k, t, slot):
        a, b, a_moves = sources_of[k]
        moving = pl.ds(pl.multiple_of(t * d, d), d)
        whole = pl.ds(0, d)
        return (
            pltpu.make_async_copy(a.at[:, moving if a_moves else whole], a_buf.at[slot], load_sem.at[slot, 0]),
            pltpu.make_async_copy(b.at[:, whole if a_moves else moving], b_buf.at[slot], load_sem.at[slot, 1]),
        )

    sources_of = [(inputs[ia], inputs[ib], moves) for ia, ib, moves in SOURCES]

    def start_load(index):
        for k in range(count):

            @pl.when(lax.div(index, tiles) == k)
            def _():
                for copy in loads(k, lax.rem(index, tiles), lax.rem(index, 2)):
                    copy.start()

    def swap(k):
        return remote(mine.at[4 + lax.rem(k, 2)], theirs.at[k], swap_send.at[k], swap_recv.at[k], partner)

    def hop(k, way, s):
        return remote(ring.at[k, way, s], ring.at[k, way, s + 1], ring_send.at[k, way, s], ring_recv.at[k, way, s], onward[way])

    def tile(index):
        k, t, slot = lax.div(index, tiles), lax.rem(index, tiles), lax.rem(index, 2)

        @pl.when(index + 1 < count * tiles)
        def _():
            start_load(index + 1)

        @pl.when(jnp.logical_and(t == 0, k >= 2))
        def _():
            swap(k - 2).wait_send()

        for copy in loads(0, 0, slot):
            copy.wait()
        down = 1 - lax.div(lax.rem(k, 3) + 1, 2)
        for part in range(2):
            cols = d // 2
            out = lax.dot_general(
                a_buf[slot, :, part * cols : (part + 1) * cols], b_buf[slot], (((0,), (0,)), ((), ())), preferred_element_type=F32
            ).astype(BF16)
            for i in range(cols // r):
                group = part * (cols // r) + i
                device = down * (t * (n // tiles) + group // tiles) + (1 - down) * group
                at = down * ((group % tiles) * d) + (1 - down) * (t * d)
                same = 1 - lax.rem(lax.rem(device, 2) + c, 2)
                buf = same * lax.rem(k, 4) + (1 - same) * (4 + lax.rem(k, 2))
                mine[buf, lax.div(device, 2), :, pl.ds(pl.multiple_of(at, d), d)] = out[i * r : (i + 1) * r]

        @pl.when(t == tiles - 1)
        def _():
            swap(k).start()

    def term(k, way, chip):
        cols = slice(way * half, (way + 1) * half)
        return mine[lax.rem(k, 4), chip, :, cols].astype(F32) + theirs[k, chip, :, cols].astype(F32)

    def meant_for(way, s):
        return lax.rem(z + chips - 1 - s, chips) if way == 0 else lax.rem(z + 1 + s, chips)

    def first(k):
        swap(k).wait_recv()
        for way in range(2):
            ring[k, way, 0] = term(k, way, meant_for(way, 0)).astype(BF16)
            hop(k, way, 0).start()

    def middle(k, s):
        for way in range(2):
            hop(k, way, s - 1).wait_recv()
            ring[k, way, s] = (term(k, way, meant_for(way, s)) + ring[k, way, s].astype(F32)).astype(BF16)
            hop(k, way, s).start()

    def last(k):
        for way in range(2):
            hop(k, way, chips - 2).wait_recv()
            g = (term(k, way, z) + ring[k, way, chips - 1].astype(F32)).astype(BF16)
            g_ref[k, :, way * half : (way + 1) * half] = g
            squares[...] += g.astype(F32) * g.astype(F32)

    start_load(0)
    squares[...] = jnp.zeros_like(squares)
    enter([lax.rem(me + o, n) for o in range(1, n)])

    @pl.loop(0, pairs + 1)
    def _(ii):
        @pl.loop(0, chips - 1)
        def _(s):
            for j in range(2):
                k = 2 * (ii - 1) + j

                @pl.when(jnp.logical_and(ii > 0, s == 0))
                def _():
                    first(k)

                @pl.when(jnp.logical_and(ii > 0, s > 0))
                def _():
                    middle(k, s)

                @pl.when(jnp.logical_and(ii > 1, s == 0))
                def _():
                    last(k - 2)

                @pl.when(jnp.logical_and(ii < pairs, s < tiles))
                def _():
                    tile(2 * tiles * ii + 2 * s + j)

    for j in range(2):
        last(jnp.int32(count - 2 + j))

    whole = squares[0:8, 0:128]
    for i in range(r // 8):
        for q in range(half // 128):
            if i or q:
                whole = whole + squares[i * 8 : (i + 1) * 8, q * 128 : (q + 1) * 128]
    slots[0] = whole
    sends = [remote(slots.at[0], slots.at[o], all_send.at[o], all_recv.at[o], lax.rem(me + o, n)) for o in range(1, n)]
    for send in sends:
        send.start()
    for send in sends:
        send.wait_recv()
    whole = slots[0]
    for o in range(1, n):
        whole = whole + slots[o]
    total_ref[...] = jnp.full(total_ref.shape, jnp.sum(whole), F32)
    for send in sends:
        send.wait_send()

    @pl.loop(0, count)
    def _(k):
        @pl.loop(0, chips - 1)
        def _(s):
            for way in range(2):
                hop(k, way, s).wait_send()

    for j in range(2):
        swap(jnp.int32(count - 2 + j)).wait_send()


SOURCES = ((0, 4, True), (1, 2, False), (1, 3, False), (5, 9, True), (6, 7, False), (6, 8, False))


def summed(n, arrays):
    tokens, d = arrays[1].shape
    ff = arrays[0].shape[1]
    r, chips, count = d // n, n // 2, len(SOURCES)
    dma = pltpu.SemaphoreType.DMA
    return pl.pallas_call(
        functools.partial(sum_kernel, n, arrays),
        out_shape=(jax.ShapeDtypeStruct((count, r, ff), BF16), jax.ShapeDtypeStruct((8, 128), F32)),
        in_specs=[pl.BlockSpec(memory_space=ANY)] * len(arrays),
        out_specs=(pl.BlockSpec(memory_space=VMEM), pl.BlockSpec(memory_space=VMEM)),
        scratch_shapes=[
            VMEM((2, tokens, d), BF16),
            VMEM((2, tokens, d), BF16),
            VMEM((6, chips, r, ff), BF16),
            VMEM((count, chips, r, ff), BF16),
            VMEM((count, 2, chips, r, ff // 2), BF16),
            VMEM((r, ff // 2), F32),
            VMEM((n, 8, 128), F32),
            dma((2, 2)),
            dma((count,)),
            dma((count,)),
            dma((count, 2, chips - 1)),
            dma((count, 2, chips - 1)),
            dma((n,)),
            dma((n,)),
        ],
        compiler_params=pltpu.CompilerParams(collective_id=0, has_side_effects=True, vmem_limit_bytes=VMEM_BYTES),
        name="gradient_sum",
    )(*arrays)


WEIGHTS = ((2, 1), (0, 1), (1, 1), (2, 0), (0, 0), (1, 0))


def pieces(k, array, block):
    name, layer = WEIGHTS[k]
    if name < 2:
        return [(array.at[layer], block)]
    tiles, width = array.shape[-3], array.shape[-1]
    lead = (slice(None),) * (len(array.shape) - 4)
    return [(array.at[(layer, *lead, q)], block.at[(*lead, slice(None), pl.ds(q * width, width))]) for q in range(tiles)]


def own_pieces(k, array, block, me):
    name, layer = WEIGHTS[k]
    if name < 2:
        return [(array.at[layer, me], block)]
    tiles, width = array.shape[-3], array.shape[-1]
    return [(array.at[layer, me, q], block.at[:, pl.ds(q * width, width)]) for q in range(tiles)]


def gather_kernel(n, g_ref, total_ref, *refs):
    w_in, m_in, v_in = (refs[i : i + 3] for i in range(0, 9, 3))
    count, r, ff = g_ref.shape
    w_out = refs[9 : 9 + count]
    m_out, v_out, w_buf, m_buf, v_buf, load_sem, store_sem, ring_send, ring_recv, pair_send, pair_recv = refs[9 + count :]
    half, chunk, chips = ff // 2, ff // 4, n // 2
    me = lax.axis_index("dp")
    z, c = lax.div(me, 2), lax.rem(me, 2)
    partner = 2 * z + 1 - c
    right = 2 * lax.rem(z + 1, chips) + c
    left = 2 * lax.rem(z + chips - 1, chips) + c
    onward = (right, left)

    def loads(k):
        name = WEIGHTS[k][0]
        parts = own_pieces(k, w_in[name], w_buf.at[k], me) + pieces(k, m_in[name], m_buf.at[k]) + pieces(k, v_in[name], v_buf.at[k])
        return [pltpu.make_async_copy(src, dst, load_sem.at[k, i]) for i, (src, dst) in enumerate(parts)]

    def stores(k):
        return (
            pltpu.make_async_copy(w_buf.at[k], w_out[k].at[me], store_sem.at[k, 0]),
            pltpu.make_async_copy(m_buf.at[k], m_out.at[k], store_sem.at[k, 1]),
            pltpu.make_async_copy(v_buf.at[k], v_out.at[k], store_sem.at[k, 2]),
        )

    def came(way, s):
        return lax.rem(z + chips - s, chips) if way == 0 else lax.rem(z + s, chips)

    def part(k, way, s):
        return w_out[k].at[2 * came(way, s) + c, :, pl.ds(way * half, half)]

    def hop(k, way, s, source=None):
        ref = part(k, way, s)
        return remote(ref if source is None else source, ref, ring_send.at[k, way, s], ring_recv.at[k, way, s], onward[way])

    def across(k, way, s, source=None):
        ref = part(k, way, s)
        return remote(ref if source is None else source, ref, pair_send.at[k, way, s], pair_recv.at[k, way, s], partner)

    for k in range(count):
        for copy in loads(k):
            copy.start()
    enter((partner, left, right))
    factor = jnp.minimum(1.0, 0.5 * lax.rsqrt(total_ref[0:1, 0:1] * (1.0 / (count * r * ff * n)) + 1e-30))

    for k in range(count):
        for copy in loads(k):
            copy.wait()

        @pl.loop(0, ff // chunk)
        def _(q):
            cols = pl.ds(pl.multiple_of(q * chunk, chunk), chunk)
            g = g_ref[k, :, cols].astype(F32) * factor
            m = 0.9 * m_buf[k, :, cols] + 0.1 * g
            v = 0.95 * v_buf[k, :, cols] + 0.05 * g * g
            w = w_buf[k, :, cols].astype(F32)
            step = m * lax.rsqrt(v + 1e-8) + 0.1 * w
            m_buf[k, :, cols] = m
            v_buf[k, :, cols] = v
            w_buf[k, :, cols] = (w - 0.02 * step).astype(BF16)

        for way in range(2):
            own = w_buf.at[k, :, pl.ds(way * half, half)]
            hop(k, way, 0, own).start()
            across(k, way, 0, own).start()
        for copy in stores(k):
            copy.start()

    @pl.loop(1, chips)
    def _(s):
        for k in range(count):
            for way in range(2):
                hop(k, way, s - 1).wait_recv()

                @pl.when(s < chips - 1)
                def _():
                    hop(k, way, s).start()

                across(k, way, s).start()

    for k in range(count):
        for copy in stores(k):
            copy.wait()

        @pl.loop(0, chips)
        def _(s):
            for way in range(2):
                across(k, way, s).wait()

                @pl.when(s < chips - 1)
                def _():
                    hop(k, way, s).wait_send()


def stepped(n, g, total, w, m, v):
    count, r, ff = g.shape
    layers, d = w[0].shape[:2]
    chips, tiles = n // 2, ff // d
    dma = pltpu.SemaphoreType.DMA
    any_spec, vmem_spec = pl.BlockSpec(memory_space=ANY), pl.BlockSpec(memory_space=VMEM)
    row = (layers, r, ff), (layers, r, ff), (layers, tiles, r, d)
    whole = (layers, n, r, ff), (layers, n, r, ff), (layers, n, tiles, r, d)
    w = [t.reshape(s) for t, s in zip(w, whole, strict=True)]
    m, v = ([t.reshape(s) for t, s in zip(ts, row, strict=True)] for ts in (m, v))
    held = pl.pallas_call(
        functools.partial(gather_kernel, n),
        out_shape=(*[VMEM((n, r, ff), BF16)] * count, VMEM((count, r, ff), F32), VMEM((count, r, ff), F32)),
        in_specs=[vmem_spec] * 2 + [any_spec] * 9,
        out_specs=(any_spec,) * (count + 2),
        scratch_shapes=[
            *[VMEM((count, r, ff), t) for t in (BF16, F32, F32)],
            dma((count, 3 * tiles)),
            dma((count, 3)),
            *[dma((count, 2, chips - 1)) for _ in range(2)],
            *[dma((count, 2, chips)) for _ in range(2)],
        ],
        compiler_params=pltpu.CompilerParams(collective_id=1, has_side_effects=True, vmem_limit_bytes=20 * 1024 * 1024),
        name="step_and_gather",
    )(g, total, *w, *m, *v)

    def write_out(*refs):
        w_held, (m_held, v_held, *outs, sem) = refs[:count], refs[count:]
        parts = [
            pair
            for k, (name, _) in enumerate(WEIGHTS)
            for out, block in ((outs[name], w_held[k]), (outs[3 + name], m_held.at[k]), (outs[6 + name], v_held.at[k]))
            for pair in pieces(k, out, block)
        ]
        copies = [pltpu.make_async_copy(block, out, sem.at[i]) for i, (out, block) in enumerate(parts)]
        for copy in copies:
            copy.start()
        for copy in copies:
            copy.wait()

    outs = pl.pallas_call(
        write_out,
        out_shape=tuple(jax.ShapeDtypeStruct(t.shape, t.dtype) for t in (*w, *m, *v)),
        in_specs=[any_spec] * (count + 2),
        out_specs=(any_spec,) * 9,
        scratch_shapes=[dma((3 * count * tiles,))],
        compiler_params=pltpu.CompilerParams(vmem_limit_bytes=1024 * 1024),
        name="write_out",
    )(*held)
    rows = (layers, d, ff), (layers, d, ff), (layers, ff, d)
    blocks = (layers, r, ff), (layers, r, ff), (layers, tiles * r, d)
    return [t.reshape(s) for t, s in zip(outs, (*rows, *blocks, *blocks), strict=True)]


def normed(h):
    wide = h.astype(F32)
    scale = lax.rsqrt(jnp.mean(wide**2, -1, keepdims=True) + 1e-6)
    return (wide * scale).astype(BF16)


def back_through_norm(h, da):
    wide, g = h.astype(F32), da.astype(F32)
    mean = jnp.mean(wide**2, -1, keepdims=True) + 1e-6
    scale = lax.rsqrt(mean)
    inner = jnp.mean(g * wide, -1, keepdims=True)
    return (scale * g - wide * (inner * scale / mean)).astype(BF16)


def back_through_product(gate, up, s, dhid):
    p = dhid.astype(BF16).astype(F32)
    return (p * up * (s * (1 + gate * (1 - s)))).astype(BF16), (p * (gate * s)).astype(BF16)


def dot(a, b):
    return jnp.dot(a, b, preferred_element_type=F32)


def dot_t(a, b):
    return lax.dot_general(a, b, (((1,), (1,)), ((), ())), preferred_element_type=F32)


def forward_kernel(chunks, x_ref, wg_ref, wu_ref, wd_ref, a_ref, hid_ref, gate_ref, up_ref, h_ref, acc):
    i = pl.program_id(0)
    size = x_ref.shape[0] // chunks

    @pl.when(i == 0)
    def _():
        a_ref[...] = normed(x_ref[...])

    for q in range(chunks):
        rows = slice(q * size, (q + 1) * size)
        gate, up = dot(a_ref[rows], wg_ref[...]), dot(a_ref[rows], wu_ref[...])
        hid = (gate * jax.nn.sigmoid(gate) * up).astype(BF16)
        gate_ref[rows], up_ref[rows], hid_ref[rows] = gate, up, hid
        more = dot(hid, wd_ref[...])

        @pl.when(i == 0)
        def _():
            acc[rows] = more

        @pl.when(i > 0)
        def _():
            acc[rows] += more

    @pl.when(i == pl.num_programs(0) - 1)
    def _():
        h_ref[...] = x_ref[...] + acc[...].astype(BF16)


def turn_kernel(chunks, h_ref, dy_ref, wg_ref, wu_ref, wd_ref, a_ref, hid_ref, dgate_ref, dup_ref, dh_ref, acc_g, acc_u):
    i = pl.program_id(0)
    size = h_ref.shape[0] // chunks

    @pl.when(i == 0)
    def _():
        a_ref[...] = normed(h_ref[...])
        acc_g[...] = jnp.zeros_like(acc_g)
        acc_u[...] = jnp.zeros_like(acc_u)

    for q in range(chunks):
        rows = slice(q * size, (q + 1) * size)
        gate, up = dot(a_ref[rows], wg_ref[...]), dot(a_ref[rows], wu_ref[...])
        dhid = dot_t(dy_ref[rows], wd_ref[...])
        s = jax.nn.sigmoid(gate)
        hid_ref[rows] = (gate * s * up).astype(BF16)
        dgate, dup = back_through_product(gate, up, s, dhid)
        dgate_ref[rows], dup_ref[rows] = dgate, dup
        acc_g[rows] += dot_t(dgate, wg_ref[...])
        acc_u[rows] += dot_t(dup, wu_ref[...])

    @pl.when(i == pl.num_programs(0) - 1)
    def _():
        da = acc_g[...].astype(BF16) + acc_u[...].astype(BF16)
        dh_ref[...] = dy_ref[...] + back_through_norm(h_ref[...], da)


def back_kernel(chunks, dy_ref, gate_ref, up_ref, wd_ref, dgate_ref, dup_ref):
    size = dy_ref.shape[0] // chunks
    for q in range(chunks):
        rows = slice(q * size, (q + 1) * size)
        gate = gate_ref[rows]
        dgate_ref[rows], dup_ref[rows] = back_through_product(gate, up_ref[rows], jax.nn.sigmoid(gate), dot_t(dy_ref[rows], wd_ref[...]))


def operands(x, dy, w_gate, w_up, w_down):
    (tokens, d), ff = x.shape, w_gate.shape[2]
    tile, chunks = ff // 6, 4
    grid = (ff // tile,)
    like = jax.ShapeDtypeStruct
    state, states = pl.BlockSpec((tokens, d), lambda i: (0, 0)), like((tokens, d), BF16)
    hidden, hiddens, wide = pl.BlockSpec((tokens, tile), lambda i: (0, i)), like((tokens, ff), BF16), like((tokens, ff), F32)

    def into(layer):
        return pl.BlockSpec((None, d, tile), lambda i: (layer, 0, i))

    def out_of(layer):
        return pl.BlockSpec((None, tile, d), lambda i: (layer, i, 0))

    acc = VMEM((tokens, d), F32)
    params = pltpu.CompilerParams(vmem_limit_bytes=56 * 1024 * 1024, dimension_semantics=("arbitrary",))
    a0, hid0, gate0, up0, h1 = pl.pallas_call(
        functools.partial(forward_kernel, chunks),
        grid=grid,
        out_shape=(states, hiddens, wide, wide, states),
        in_specs=[state, into(0), into(0), out_of(0)],
        out_specs=(state, hidden, hidden, hidden, state),
        scratch_shapes=[acc],
        compiler_params=params,
        name="first_forward",
    )(x, w_gate, w_up, w_down)
    a1, hid1, dgate1, dup1, dy0 = pl.pallas_call(
        functools.partial(turn_kernel, chunks),
        grid=grid,
        out_shape=(states, hiddens, hiddens, hiddens, states),
        in_specs=[state, state, into(1), into(1), out_of(1)],
        out_specs=(state, hidden, hidden, hidden, state),
        scratch_shapes=[acc, acc],
        compiler_params=params,
        name="last_layer",
    )(h1, dy, w_gate, w_up, w_down)
    dgate0, dup0 = pl.pallas_call(
        functools.partial(back_kernel, chunks),
        grid=grid,
        out_shape=(hiddens, hiddens),
        in_specs=[state, hidden, hidden, out_of(0)],
        out_specs=(hidden, hidden),
        compiler_params=params,
        name="first_back",
    )(dy0, gate0, up0, w_down)
    return hid1, a1, dgate1, dup1, dy, hid0, a0, dgate0, dup0, dy0


def solution(mesh):
    n = mesh.shape["dp"]

    def device(x, dy, *arrays):
        w, m, v = (arrays[i : i + 3] for i in (0, 3, 6))
        g, total = summed(n, operands(x[0], dy[0], *w))
        return tuple(stepped(n, g, total, w, m, v))

    whole, rows = P(None, None, None), P(None, "dp", None)
    tokens = P(("rep", "dp"), None, None)
    return jax.shard_map(
        device,
        mesh=mesh,
        in_specs=(tokens, tokens, *[whole] * 3, *[rows] * 6),
        out_specs=(*[P("rep", None, None)] * 3, *[P("rep", "dp", None)] * 6),
        check_vma=False,
    )
```

```python
import functools

import jax
import jax.numpy as jnp
from jax import lax
from jax.experimental import pallas as pl
from jax.experimental.pallas import tpu as pltpu
from jax.sharding import PartitionSpec as P

F32, BF16 = jnp.float32, jnp.bfloat16
ANY, VMEM = pl.ANY, pltpu.VMEM
MESH = pl.DeviceIdType.MESH
VMEM_BYTES = 64 * 1024 * 1024 - 65536


def remote(src, dst, send, recv, to):
    return pltpu.make_async_remote_copy(
        src_ref=src, dst_ref=dst, send_sem=send, recv_sem=recv, device_id={"dp": to}, device_id_type=MESH
    )


def enter(peers):
    barrier = pltpu.get_barrier_semaphore()
    for peer in peers:
        pl.semaphore_signal(barrier, inc=1, device_id={"dp": peer}, device_id_type=MESH)
    pl.semaphore_wait(barrier, len(peers))


def sum_kernel(n, inputs_count, *refs):
    *inputs, wg, wu, wd = refs[:inputs_count]
    g_ref, total_ref, dgate, dup = refs[inputs_count : inputs_count + 4]
    (a_buf, b_buf, wg_buf, wu_buf, wd_buf, mine, theirs, ring, squares, slots, *sems) = refs[inputs_count + 4 :]
    load_sem, back_sem, swap_send, swap_recv, ring_send, ring_recv, all_send, all_recv = sems
    inputs += [dgate, dup]
    d = a_buf.shape[2]
    r, ff = mine.shape[2:]
    half, tiles, chips = ff // 2, ff // d, n // 2
    width = wg_buf.shape[1]
    backs = ff // width
    late = backs - (chips - 1 - tiles)
    shift = 2 * late - 1
    count = ring.shape[0]
    pairs = count // 2
    me = lax.axis_index("dp")
    z, c = lax.div(me, 2), lax.rem(me, 2)
    partner = 2 * z + 1 - c
    right = 2 * lax.rem(z + 1, chips) + c
    left = 2 * lax.rem(z + chips - 1, chips) + c
    onward = (right, left)

    def loads(k, t, slot):
        a, b, a_moves = sources_of[k]
        moving = pl.ds(pl.multiple_of(t * d, d), d)
        whole = pl.ds(0, d)
        return (
            pltpu.make_async_copy(a.at[:, moving if a_moves else whole], a_buf.at[slot], load_sem.at[slot, 0]),
            pltpu.make_async_copy(b.at[:, whole if a_moves else moving], b_buf.at[slot], load_sem.at[slot, 1]),
        )

    sources_of = [(inputs[ia], inputs[ib], moves) for ia, ib, moves in SOURCES]

    def back_loads(u):
        at = pl.ds(pl.multiple_of(u * width, width), width)
        return (
            pltpu.make_async_copy(wg.at[0, :, at], wg_buf, back_sem.at[0]),
            pltpu.make_async_copy(wu.at[0, :, at], wu_buf, back_sem.at[1]),
            pltpu.make_async_copy(wd.at[0, at], wd_buf, back_sem.at[2]),
        )

    def back_states():
        return (
            pltpu.make_async_copy(inputs[A0], a_buf.at[0], back_sem.at[3]),
            pltpu.make_async_copy(inputs[DY0], b_buf.at[0], back_sem.at[4]),
        )

    def back_stores(u):
        at = pl.ds(pl.multiple_of(u * width, width), width)
        return (
            pltpu.make_async_copy(a_buf.at[1, :, pl.ds(0, width)], dgate.at[:, at], back_sem.at[5]),
            pltpu.make_async_copy(b_buf.at[1, :, pl.ds(0, width)], dup.at[:, at], back_sem.at[6]),
        )

    def back(u):
        @pl.when(u == 0)
        def _():
            for copy in back_states():
                copy.wait()

        @pl.when(u > 0)
        def _():
            for copy in back_stores(u - 1):
                copy.wait()

        for copy in back_loads(u):
            copy.wait()
        size = a_buf.shape[1] // 4
        for q in range(4):
            rows = slice(q * size, (q + 1) * size)
            gate, up = dot(a_buf[0, rows], wg_buf[...]), dot(a_buf[0, rows], wu_buf[...])
            dhid = dot_t(b_buf[0, rows], wd_buf[...])
            a_buf[1, rows, :width], b_buf[1, rows, :width] = back_through_product(gate, up, jax.nn.sigmoid(gate), dhid)
        for copy in back_stores(u):
            copy.start()

        @pl.when(u + 1 < backs)
        def _():
            for copy in back_loads(u + 1):
                copy.start()

        @pl.when(u + 1 == backs)
        def _():
            for copy in back_stores(u):
                copy.wait()
            start_load(jnp.int32(2 * tiles * 2))

    def start_load(index):
        for k in range(count):

            @pl.when(lax.div(index, tiles) == k)
            def _():
                for copy in loads(k, lax.rem(index, tiles), lax.rem(index, 2)):
                    copy.start()

    def swap(k):
        return remote(mine.at[4 + lax.rem(k, 2)], theirs.at[k], swap_send.at[k], swap_recv.at[k], partner)

    def hop(k, way, s):
        return remote(ring.at[k, way, s], ring.at[k, way, s + 1], ring_send.at[k, way, s], ring_recv.at[k, way, s], onward[way])

    def tile(index):
        k, t, slot = lax.div(index, tiles), lax.rem(index, tiles), lax.rem(index, 2)

        @pl.when(jnp.logical_and(index + 1 < count * tiles, index + 1 != 4 * tiles))
        def _():
            start_load(index + 1)

        @pl.when(index + 1 == 4 * tiles)
        def _():
            for copy in back_loads(jnp.int32(0)):
                copy.start()

        @pl.when(jnp.logical_and(t == 0, k >= 2))
        def _():
            swap(k - 2).wait_send()

        for copy in loads(0, 0, slot):
            copy.wait()
        down = 1 - lax.div(lax.rem(k, 3) + 1, 2)
        for part in range(2):
            cols = d // 2
            out = lax.dot_general(
                a_buf[slot, :, part * cols : (part + 1) * cols], b_buf[slot], (((0,), (0,)), ((), ())), preferred_element_type=F32
            ).astype(BF16)
            for i in range(cols // r):
                group = part * (cols // r) + i
                device = down * (t * (n // tiles) + group // tiles) + (1 - down) * group
                at = down * ((group % tiles) * d) + (1 - down) * (t * d)
                same = 1 - lax.rem(lax.rem(device, 2) + c, 2)
                buf = same * lax.rem(k, 4) + (1 - same) * (4 + lax.rem(k, 2))
                mine[buf, lax.div(device, 2), :, pl.ds(pl.multiple_of(at, d), d)] = out[i * r : (i + 1) * r]

        @pl.when(t == tiles - 1)
        def _():
            swap(k).start()

    def term(k, way, chip):
        cols = slice(way * half, (way + 1) * half)
        return mine[lax.rem(k, 4), chip, :, cols].astype(F32) + theirs[k, chip, :, cols].astype(F32)

    def meant_for(way, s):
        return lax.rem(z + chips - 1 - s, chips) if way == 0 else lax.rem(z + 1 + s, chips)

    def first(k):
        swap(k).wait_recv()
        for way in range(2):
            ring[k, way, 0] = term(k, way, meant_for(way, 0)).astype(BF16)
            hop(k, way, 0).start()

    def middle(k, s):
        for way in range(2):
            hop(k, way, s - 1).wait_recv()
            ring[k, way, s] = (term(k, way, meant_for(way, s)) + ring[k, way, s].astype(F32)).astype(BF16)
            hop(k, way, s).start()

    def last(k):
        for way in range(2):
            hop(k, way, chips - 2).wait_recv()
            g = (term(k, way, z) + ring[k, way, chips - 1].astype(F32)).astype(BF16)
            g_ref[k, :, way * half : (way + 1) * half] = g
            squares[...] += g.astype(F32) * g.astype(F32)

    start_load(0)
    squares[...] = jnp.zeros_like(squares)
    enter([lax.rem(me + o, n) for o in range(1, n)])

    @pl.loop(0, pairs + 1)
    def _(ii):
        @pl.loop(0, chips - 1)
        def _(s):
            for j in range(2):
                k = 2 * (ii - 1) + j

                @pl.when(jnp.logical_and(ii > 0, s == 0))
                def _():
                    first(k)

                @pl.when(jnp.logical_and(ii > 0, s > 0))
                def _():
                    middle(k, s)

                @pl.when(jnp.logical_and(ii > 1, s == 0))
                def _():
                    last(k - 2)

                place = 2 * s + j - shift * lax.div(ii, 2)

                @pl.when(jnp.logical_and(ii < pairs, jnp.logical_and(place >= 0, place < 2 * tiles)))
                def _():
                    tile(2 * tiles * ii + place)

                if j == 0:

                    @pl.when(jnp.logical_and(ii == 1, s == tiles))
                    def _():
                        for copy in back_states():
                            copy.start()

                if j == 0:
                    due, u = jnp.logical_and(ii == 2, s == late - 1), jnp.int32(backs - 1)
                else:
                    due = jnp.logical_or(jnp.logical_and(ii == 1, s >= tiles), jnp.logical_and(ii == 2, s < late - 1))
                    u = s - tiles + (ii - 1) * (chips - 1)

                @pl.when(due)
                def _():
                    back(u)

    for j in range(2):
        last(jnp.int32(count - 2 + j))

    whole = squares[0:8, 0:128]
    for i in range(r // 8):
        for q in range(half // 128):
            if i or q:
                whole = whole + squares[i * 8 : (i + 1) * 8, q * 128 : (q + 1) * 128]
    slots[0] = whole
    sends = [remote(slots.at[0], slots.at[o], all_send.at[o], all_recv.at[o], lax.rem(me + o, n)) for o in range(1, n)]
    for send in sends:
        send.start()
    for send in sends:
        send.wait_recv()
    whole = slots[0]
    for o in range(1, n):
        whole = whole + slots[o]
    total_ref[...] = jnp.full(total_ref.shape, jnp.sum(whole), F32)
    for send in sends:
        send.wait_send()

    @pl.loop(0, count)
    def _(k):
        @pl.loop(0, chips - 1)
        def _(s):
            for way in range(2):
                hop(k, way, s).wait_send()

    for j in range(2):
        swap(jnp.int32(count - 2 + j)).wait_send()


SOURCES = ((0, 4, True), (1, 2, False), (1, 3, False), (5, 7, True), (6, 8, False), (6, 9, False))
A0, DY0 = 6, 7


def summed(n, arrays, weights):
    tokens, d = arrays[1].shape
    ff = arrays[0].shape[1]
    r, chips, count, width = d // n, n // 2, len(SOURCES), ff // 6
    dma = pltpu.SemaphoreType.DMA
    like, any_spec, vmem_spec = jax.ShapeDtypeStruct, pl.BlockSpec(memory_space=ANY), pl.BlockSpec(memory_space=VMEM)
    operands = (*arrays, *weights)
    return pl.pallas_call(
        functools.partial(sum_kernel, n, len(operands)),
        out_shape=(like((count, r, ff), BF16), like((8, 128), F32), like((tokens, ff), BF16), like((tokens, ff), BF16)),
        in_specs=[any_spec] * len(operands),
        out_specs=(vmem_spec, vmem_spec, any_spec, any_spec),
        scratch_shapes=[
            VMEM((2, tokens, d), BF16),
            VMEM((2, tokens, d), BF16),
            VMEM((d, width), BF16),
            VMEM((d, width), BF16),
            VMEM((width, d), BF16),
            VMEM((6, chips, r, ff), BF16),
            VMEM((count, chips, r, ff), BF16),
            VMEM((count, 2, chips, r, ff // 2), BF16),
            VMEM((r, ff // 2), F32),
            VMEM((n, 8, 128), F32),
            dma((2, 2)),
            dma((7,)),
            dma((count,)),
            dma((count,)),
            dma((count, 2, chips - 1)),
            dma((count, 2, chips - 1)),
            dma((n,)),
            dma((n,)),
        ],
        compiler_params=pltpu.CompilerParams(collective_id=0, has_side_effects=True, vmem_limit_bytes=VMEM_BYTES),
        name="gradient_sum",
    )(*operands)


WEIGHTS = ((2, 1), (0, 1), (1, 1), (2, 0), (0, 0), (1, 0))


def pieces(k, array, block):
    name, layer = WEIGHTS[k]
    if name < 2:
        return [(array.at[layer], block)]
    tiles, width = array.shape[-3], array.shape[-1]
    lead = (slice(None),) * (len(array.shape) - 4)
    return [(array.at[(layer, *lead, q)], block.at[(*lead, slice(None), pl.ds(q * width, width))]) for q in range(tiles)]


def own_pieces(k, array, block, me):
    name, layer = WEIGHTS[k]
    if name < 2:
        return [(array.at[layer, me], block)]
    tiles, width = array.shape[-3], array.shape[-1]
    return [(array.at[layer, me, q], block.at[:, pl.ds(q * width, width)]) for q in range(tiles)]


def gather_kernel(n, g_ref, total_ref, *refs):
    w_in, m_in, v_in = (refs[i : i + 3] for i in range(0, 9, 3))
    count, r, ff = g_ref.shape
    w_out = refs[9 : 9 + count]
    m_out, v_out, w_buf, m_buf, v_buf, load_sem, store_sem, ring_send, ring_recv, pair_send, pair_recv = refs[9 + count :]
    half, chunk, chips = ff // 2, ff // 4, n // 2
    me = lax.axis_index("dp")
    z, c = lax.div(me, 2), lax.rem(me, 2)
    partner = 2 * z + 1 - c
    right = 2 * lax.rem(z + 1, chips) + c
    left = 2 * lax.rem(z + chips - 1, chips) + c
    onward = (right, left)

    def loads(k):
        name = WEIGHTS[k][0]
        parts = own_pieces(k, w_in[name], w_buf.at[k], me) + pieces(k, m_in[name], m_buf.at[k]) + pieces(k, v_in[name], v_buf.at[k])
        return [pltpu.make_async_copy(src, dst, load_sem.at[k, i]) for i, (src, dst) in enumerate(parts)]

    def stores(k):
        return (
            pltpu.make_async_copy(w_buf.at[k], w_out[k].at[me], store_sem.at[k, 0]),
            pltpu.make_async_copy(m_buf.at[k], m_out.at[k], store_sem.at[k, 1]),
            pltpu.make_async_copy(v_buf.at[k], v_out.at[k], store_sem.at[k, 2]),
        )

    def came(way, s):
        return lax.rem(z + chips - s, chips) if way == 0 else lax.rem(z + s, chips)

    def part(k, way, s):
        return w_out[k].at[2 * came(way, s) + c, :, pl.ds(way * half, half)]

    def hop(k, way, s, source=None):
        ref = part(k, way, s)
        return remote(ref if source is None else source, ref, ring_send.at[k, way, s], ring_recv.at[k, way, s], onward[way])

    def across(k, way, s, source=None):
        ref = part(k, way, s)
        return remote(ref if source is None else source, ref, pair_send.at[k, way, s], pair_recv.at[k, way, s], partner)

    for k in range(count):
        for copy in loads(k):
            copy.start()
    enter((partner, left, right))
    factor = jnp.minimum(1.0, 0.5 * lax.rsqrt(total_ref[0:1, 0:1] * (1.0 / (count * r * ff * n)) + 1e-30))

    for k in range(count):
        for copy in loads(k):
            copy.wait()

        @pl.loop(0, ff // chunk)
        def _(q):
            cols = pl.ds(pl.multiple_of(q * chunk, chunk), chunk)
            g = g_ref[k, :, cols].astype(F32) * factor
            m = 0.9 * m_buf[k, :, cols] + 0.1 * g
            v = 0.95 * v_buf[k, :, cols] + 0.05 * g * g
            w = w_buf[k, :, cols].astype(F32)
            step = m * lax.rsqrt(v + 1e-8) + 0.1 * w
            m_buf[k, :, cols] = m
            v_buf[k, :, cols] = v
            w_buf[k, :, cols] = (w - 0.02 * step).astype(BF16)

        for way in range(2):
            own = w_buf.at[k, :, pl.ds(way * half, half)]
            hop(k, way, 0, own).start()
            across(k, way, 0, own).start()
        for copy in stores(k):
            copy.start()

    @pl.loop(1, chips)
    def _(s):
        for k in range(count):
            for way in range(2):
                hop(k, way, s - 1).wait_recv()

                @pl.when(s < chips - 1)
                def _():
                    hop(k, way, s).start()

                across(k, way, s).start()

    for k in range(count):
        for copy in stores(k):
            copy.wait()

        @pl.loop(0, chips)
        def _(s):
            for way in range(2):
                across(k, way, s).wait()

                @pl.when(s < chips - 1)
                def _():
                    hop(k, way, s).wait_send()


def stepped(n, g, total, w, m, v):
    count, r, ff = g.shape
    layers, d = w[0].shape[:2]
    chips, tiles = n // 2, ff // d
    dma = pltpu.SemaphoreType.DMA
    any_spec, vmem_spec = pl.BlockSpec(memory_space=ANY), pl.BlockSpec(memory_space=VMEM)
    row = (layers, r, ff), (layers, r, ff), (layers, tiles, r, d)
    whole = (layers, n, r, ff), (layers, n, r, ff), (layers, n, tiles, r, d)
    w = [t.reshape(s) for t, s in zip(w, whole, strict=True)]
    m, v = ([t.reshape(s) for t, s in zip(ts, row, strict=True)] for ts in (m, v))
    held = pl.pallas_call(
        functools.partial(gather_kernel, n),
        out_shape=(*[VMEM((n, r, ff), BF16)] * count, *[jax.ShapeDtypeStruct((count, r, ff), F32)] * 2),
        in_specs=[vmem_spec] * 2 + [any_spec] * 9,
        out_specs=(any_spec,) * (count + 2),
        scratch_shapes=[
            *[VMEM((count, r, ff), t) for t in (BF16, F32, F32)],
            dma((count, 3 * tiles)),
            dma((count, 3)),
            *[dma((count, 2, chips - 1)) for _ in range(2)],
            *[dma((count, 2, chips)) for _ in range(2)],
        ],
        compiler_params=pltpu.CompilerParams(collective_id=1, has_side_effects=True, vmem_limit_bytes=20 * 1024 * 1024),
        name="step_and_gather",
    )(g, total, *w, *m, *v)

    def write_out(*refs):
        w_held, (m_held, v_held, *outs, sem) = refs[:count], refs[count:]
        parts = [
            pair
            for k, (name, _) in enumerate(WEIGHTS)
            for out, block in ((outs[name], w_held[k]), (outs[3 + name], m_held.at[k]), (outs[6 + name], v_held.at[k]))
            for pair in pieces(k, out, block)
        ]
        copies = [pltpu.make_async_copy(block, out, sem.at[i]) for i, (out, block) in enumerate(parts)]
        for copy in copies:
            copy.start()
        for copy in copies:
            copy.wait()

    outs = pl.pallas_call(
        write_out,
        out_shape=tuple(jax.ShapeDtypeStruct(t.shape, t.dtype) for t in (*w, *m, *v)),
        in_specs=[any_spec] * (count + 2),
        out_specs=(any_spec,) * 9,
        scratch_shapes=[dma((3 * count * tiles,))],
        compiler_params=pltpu.CompilerParams(vmem_limit_bytes=1024 * 1024),
        name="write_out",
    )(*held)
    rows = (layers, d, ff), (layers, d, ff), (layers, ff, d)
    blocks = (layers, r, ff), (layers, r, ff), (layers, tiles * r, d)
    return [t.reshape(s) for t, s in zip(outs, (*rows, *blocks, *blocks), strict=True)]


def normed(h):
    wide = h.astype(F32)
    scale = lax.rsqrt(jnp.mean(wide**2, -1, keepdims=True) + 1e-6)
    return (wide * scale).astype(BF16)


def back_through_norm(h, da):
    wide, g = h.astype(F32), da.astype(F32)
    mean = jnp.mean(wide**2, -1, keepdims=True) + 1e-6
    scale = lax.rsqrt(mean)
    inner = jnp.mean(g * wide, -1, keepdims=True)
    return (scale * g - wide * (inner * scale / mean)).astype(BF16)


def back_through_product(gate, up, s, dhid):
    p = dhid.astype(BF16).astype(F32)
    return (p * up * (s * (1 + gate * (1 - s)))).astype(BF16), (p * (gate * s)).astype(BF16)


def dot(a, b):
    return jnp.dot(a, b, preferred_element_type=F32)


def dot_t(a, b):
    return lax.dot_general(a, b, (((1,), (1,)), ((), ())), preferred_element_type=F32)


def forward_kernel(chunks, x_ref, wg_ref, wu_ref, wd_ref, a_ref, hid_ref, h_ref, acc):
    i = pl.program_id(0)
    size = x_ref.shape[0] // chunks

    @pl.when(i == 0)
    def _():
        a_ref[...] = normed(x_ref[...])

    for q in range(chunks):
        rows = slice(q * size, (q + 1) * size)
        gate, up = dot(a_ref[rows], wg_ref[...]), dot(a_ref[rows], wu_ref[...])
        hid = (gate * jax.nn.sigmoid(gate) * up).astype(BF16)
        hid_ref[rows] = hid
        more = dot(hid, wd_ref[...])

        @pl.when(i == 0)
        def _():
            acc[rows] = more

        @pl.when(i > 0)
        def _():
            acc[rows] += more

    @pl.when(i == pl.num_programs(0) - 1)
    def _():
        h_ref[...] = x_ref[...] + acc[...].astype(BF16)


def turn_kernel(chunks, h_ref, dy_ref, wg_ref, wu_ref, wd_ref, a_ref, hid_ref, dgate_ref, dup_ref, dh_ref, acc_g, acc_u):
    i = pl.program_id(0)
    size = h_ref.shape[0] // chunks

    @pl.when(i == 0)
    def _():
        a_ref[...] = normed(h_ref[...])
        acc_g[...] = jnp.zeros_like(acc_g)
        acc_u[...] = jnp.zeros_like(acc_u)

    for q in range(chunks):
        rows = slice(q * size, (q + 1) * size)
        gate, up = dot(a_ref[rows], wg_ref[...]), dot(a_ref[rows], wu_ref[...])
        dhid = dot_t(dy_ref[rows], wd_ref[...])
        s = jax.nn.sigmoid(gate)
        hid_ref[rows] = (gate * s * up).astype(BF16)
        dgate, dup = back_through_product(gate, up, s, dhid)
        dgate_ref[rows], dup_ref[rows] = dgate, dup
        acc_g[rows] += dot_t(dgate, wg_ref[...])
        acc_u[rows] += dot_t(dup, wu_ref[...])

    @pl.when(i == pl.num_programs(0) - 1)
    def _():
        da = acc_g[...].astype(BF16) + acc_u[...].astype(BF16)
        dh_ref[...] = dy_ref[...] + back_through_norm(h_ref[...], da)


def operands(x, dy, w_gate, w_up, w_down):
    (tokens, d), ff = x.shape, w_gate.shape[2]
    tile, chunks = ff // 6, 4
    grid = (ff // tile,)
    like = jax.ShapeDtypeStruct
    state, states = pl.BlockSpec((tokens, d), lambda i: (0, 0)), like((tokens, d), BF16)
    hidden, hiddens = pl.BlockSpec((tokens, tile), lambda i: (0, i)), like((tokens, ff), BF16)

    def into(layer):
        return pl.BlockSpec((None, d, tile), lambda i: (layer, 0, i))

    def out_of(layer):
        return pl.BlockSpec((None, tile, d), lambda i: (layer, i, 0))

    acc = VMEM((tokens, d), F32)
    params = pltpu.CompilerParams(vmem_limit_bytes=56 * 1024 * 1024, dimension_semantics=("arbitrary",))
    a0, hid0, h1 = pl.pallas_call(
        functools.partial(forward_kernel, chunks),
        grid=grid,
        out_shape=(states, hiddens, states),
        in_specs=[state, into(0), into(0), out_of(0)],
        out_specs=(state, hidden, state),
        scratch_shapes=[acc],
        compiler_params=params,
        name="first_forward",
    )(x, w_gate, w_up, w_down)
    a1, hid1, dgate1, dup1, dy0 = pl.pallas_call(
        functools.partial(turn_kernel, chunks),
        grid=grid,
        out_shape=(states, hiddens, hiddens, hiddens, states),
        in_specs=[state, state, into(1), into(1), out_of(1)],
        out_specs=(state, hidden, hidden, hidden, state),
        scratch_shapes=[acc, acc],
        compiler_params=params,
        name="last_layer",
    )(h1, dy, w_gate, w_up, w_down)
    return hid1, a1, dgate1, dup1, dy, hid0, a0, dy0


def solution(mesh):
    n = mesh.shape["dp"]

    def device(x, dy, *arrays):
        w, m, v = (arrays[i : i + 3] for i in (0, 3, 6))
        g, total, *_ = summed(n, operands(x[0], dy[0], *w), w)
        return tuple(stepped(n, g, total, w, m, v))

    whole, rows = P(None, None, None), P(None, "dp", None)
    tokens = P(("rep", "dp"), None, None)
    return jax.shard_map(
        device,
        mesh=mesh,
        in_specs=(tokens, tokens, *[whole] * 3, *[rows] * 6),
        out_specs=(*[P("rep", None, None)] * 3, *[P("rep", "dp", None)] * 6),
        check_vma=False,
    )
```

```python
import functools

import jax
import jax.numpy as jnp
from jax import lax
from jax.experimental import pallas as pl
from jax.experimental.pallas import tpu as pltpu
from jax.sharding import PartitionSpec as P

F32, BF16 = jnp.float32, jnp.bfloat16
ANY, HBM, VMEM = pl.ANY, pltpu.HBM, pltpu.VMEM
MESH = pl.DeviceIdType.MESH
VMEM_BYTES = 64 * 1024 * 1024 - 65536


def remote(src, dst, send, recv, to):
    return pltpu.make_async_remote_copy(
        src_ref=src, dst_ref=dst, send_sem=send, recv_sem=recv, device_id={"dp": to}, device_id_type=MESH
    )


def enter(peers):
    for peer in peers:
        pl.semaphore_signal(pltpu.get_barrier_semaphore(), inc=1, device_id={"dp": peer}, device_id_type=MESH)


def meet(count):
    pl.semaphore_wait(pltpu.get_barrier_semaphore(), count)


def sum_kernel(n, inputs_count, *refs):
    *inputs, wg, wu, wd = refs[:inputs_count]
    g_ref, total_ref, dgate, dup = refs[inputs_count : inputs_count + 4]
    (a_buf, b_buf, wg_buf, wu_buf, wd_buf, mine, theirs, ring, squares, slots, *sems) = refs[inputs_count + 4 :]
    load_sem, back_sem, swap_send, swap_recv, ring_send, ring_recv, all_send, all_recv = sems
    inputs += [dgate, dup]
    d = a_buf.shape[2]
    r, ff = mine.shape[2:]
    half, tiles, chips = ff // 2, ff // d, n // 2
    width = wg_buf.shape[1]
    backs = ff // width
    late = backs - (chips - 1 - tiles)
    shift = 2 * late - 1
    count = ring.shape[0]
    pairs = count // 2
    me = lax.axis_index("dp")
    z, c = lax.div(me, 2), lax.rem(me, 2)
    partner = 2 * z + 1 - c
    right = 2 * lax.rem(z + 1, chips) + c
    left = 2 * lax.rem(z + chips - 1, chips) + c
    onward = (right, left)

    def loads(k, t, slot):
        a, b, a_moves = sources_of[k]
        moving = pl.ds(pl.multiple_of(t * d, d), d)
        whole = pl.ds(0, d)
        return (
            pltpu.make_async_copy(a.at[:, moving if a_moves else whole], a_buf.at[slot], load_sem.at[slot, 0]),
            pltpu.make_async_copy(b.at[:, whole if a_moves else moving], b_buf.at[slot], load_sem.at[slot, 1]),
        )

    sources_of = [(inputs[ia], inputs[ib], moves) for ia, ib, moves in SOURCES]

    def back_loads(u):
        at = pl.ds(pl.multiple_of(u * width, width), width)
        return (
            pltpu.make_async_copy(wg.at[0, :, at], wg_buf, back_sem.at[0]),
            pltpu.make_async_copy(wu.at[0, :, at], wu_buf, back_sem.at[1]),
            pltpu.make_async_copy(wd.at[0, at], wd_buf, back_sem.at[2]),
        )

    def back_states():
        return (
            pltpu.make_async_copy(inputs[A0], a_buf.at[0], back_sem.at[3]),
            pltpu.make_async_copy(inputs[DY0], b_buf.at[0], back_sem.at[4]),
        )

    def back_stores(u):
        at = pl.ds(pl.multiple_of(u * width, width), width)
        return (
            pltpu.make_async_copy(a_buf.at[1, :, pl.ds(0, width)], dgate.at[:, at], back_sem.at[5]),
            pltpu.make_async_copy(b_buf.at[1, :, pl.ds(0, width)], dup.at[:, at], back_sem.at[6]),
        )

    def back(u):
        @pl.when(u == 0)
        def _():
            for copy in back_states():
                copy.wait()

        @pl.when(u > 0)
        def _():
            for copy in back_stores(u - 1):
                copy.wait()

        for copy in back_loads(u):
            copy.wait()
        size = a_buf.shape[1] // 4
        for q in range(4):
            rows = slice(q * size, (q + 1) * size)
            gate, up = dot(a_buf[0, rows], wg_buf[...]), dot(a_buf[0, rows], wu_buf[...])
            dhid = dot_t(b_buf[0, rows], wd_buf[...])
            a_buf[1, rows, :width], b_buf[1, rows, :width] = back_through_product(gate, up, jax.nn.sigmoid(gate), dhid)
        for copy in back_stores(u):
            copy.start()

        @pl.when(u + 1 < backs)
        def _():
            for copy in back_loads(u + 1):
                copy.start()

        @pl.when(u + 1 == backs)
        def _():
            for copy in back_stores(u):
                copy.wait()
            start_load(jnp.int32(2 * tiles * 2))

    def start_load(index):
        for k in range(count):

            @pl.when(lax.div(index, tiles) == k)
            def _():
                for copy in loads(k, lax.rem(index, tiles), lax.rem(index, 2)):
                    copy.start()

    def swap(k):
        return remote(mine.at[4 + lax.rem(k, 2)], theirs.at[k], swap_send.at[k], swap_recv.at[k], partner)

    def hop(k, way, s):
        return remote(ring.at[k, way, s], ring.at[k, way, s + 1], ring_send.at[k, way, s], ring_recv.at[k, way, s], onward[way])

    def tile(index, swaps=True):
        k, t, slot = lax.div(index, tiles), lax.rem(index, tiles), lax.rem(index, 2)

        @pl.when(jnp.logical_and(index + 1 < count * tiles, index + 1 != 4 * tiles))
        def _():
            start_load(index + 1)

        @pl.when(index + 1 == 4 * tiles)
        def _():
            for copy in back_loads(jnp.int32(0)):
                copy.start()

        @pl.when(jnp.logical_and(t == 0, k >= 2))
        def _():
            swap(k - 2).wait_send()

        for copy in loads(0, 0, slot):
            copy.wait()
        down = 1 - lax.div(lax.rem(k, 3) + 1, 2)
        for part in range(2):
            cols = d // 2
            out = lax.dot_general(
                a_buf[slot, :, part * cols : (part + 1) * cols], b_buf[slot], (((0,), (0,)), ((), ())), preferred_element_type=F32
            ).astype(BF16)
            for i in range(cols // r):
                group = part * (cols // r) + i
                device = down * (t * (n // tiles) + group // tiles) + (1 - down) * group
                at = down * ((group % tiles) * d) + (1 - down) * (t * d)
                same = 1 - lax.rem(lax.rem(device, 2) + c, 2)
                buf = same * lax.rem(k, 4) + (1 - same) * (4 + lax.rem(k, 2))
                mine[buf, lax.div(device, 2), :, pl.ds(pl.multiple_of(at, d), d)] = out[i * r : (i + 1) * r]

        if swaps:

            @pl.when(t == tiles - 1)
            def _():
                swap(k).start()

    def term(k, way, chip):
        cols = slice(way * half, (way + 1) * half)
        return mine[lax.rem(k, 4), chip, :, cols].astype(F32) + theirs[k, chip, :, cols].astype(F32)

    def meant_for(way, s):
        return lax.rem(z + chips - 1 - s, chips) if way == 0 else lax.rem(z + 1 + s, chips)

    def first(k):
        swap(k).wait_recv()
        for way in range(2):
            ring[k, way, 0] = term(k, way, meant_for(way, 0)).astype(BF16)
            hop(k, way, 0).start()

    def middle(k, s):
        for way in range(2):
            hop(k, way, s - 1).wait_recv()
            ring[k, way, s] = (term(k, way, meant_for(way, s)) + ring[k, way, s].astype(F32)).astype(BF16)
            hop(k, way, s).start()

    def last(k):
        for way in range(2):
            hop(k, way, chips - 2).wait_recv()
            g = (term(k, way, z) + ring[k, way, chips - 1].astype(F32)).astype(BF16)
            g_ref[k, :, way * half : (way + 1) * half] = g
            squares[...] += g.astype(F32) * g.astype(F32)

    enter([lax.rem(me + o, n) for o in range(1, n)])
    start_load(0)
    squares[...] = jnp.zeros_like(squares)

    @pl.loop(0, tiles)
    def _(index):
        tile(index, swaps=False)

    meet(n - 1)
    swap(jnp.int32(0)).start()

    @pl.loop(0, pairs + 1)
    def _(ii):
        @pl.loop(0, chips - 1)
        def _(s):
            for j in range(2):
                k = 2 * (ii - 1) + j

                @pl.when(jnp.logical_and(ii > 0, s == 0))
                def _():
                    first(k)

                @pl.when(jnp.logical_and(ii > 0, s > 0))
                def _():
                    middle(k, s)

                @pl.when(jnp.logical_and(ii > 1, s == 0))
                def _():
                    last(k - 2)

                place = 2 * s + j - shift * lax.div(ii, 2)

                @pl.when(jnp.logical_and(ii < pairs, jnp.logical_and(place >= tiles * (1 - lax.div(ii + 2, 3)), place < 2 * tiles)))
                def _():
                    tile(2 * tiles * ii + place)

                if j == 0:

                    @pl.when(jnp.logical_and(ii == 1, s == tiles))
                    def _():
                        for copy in back_states():
                            copy.start()

                if j == 0:
                    due, u = jnp.logical_and(ii == 2, s == late - 1), jnp.int32(backs - 1)
                else:
                    due = jnp.logical_or(jnp.logical_and(ii == 1, s >= tiles), jnp.logical_and(ii == 2, s < late - 1))
                    u = s - tiles + (ii - 1) * (chips - 1)

                @pl.when(due)
                def _():
                    back(u)

    for j in range(2):
        last(jnp.int32(count - 2 + j))

    whole = squares[0:8, 0:128]
    for i in range(r // 8):
        for q in range(half // 128):
            if i or q:
                whole = whole + squares[i * 8 : (i + 1) * 8, q * 128 : (q + 1) * 128]
    slots[0] = whole
    sends = [remote(slots.at[0], slots.at[o], all_send.at[o], all_recv.at[o], lax.rem(me + o, n)) for o in range(1, n)]
    for send in sends:
        send.start()
    for send in sends:
        send.wait_recv()
    whole = slots[0]
    for o in range(1, n):
        whole = whole + slots[o]
    total_ref[...] = jnp.full(total_ref.shape, jnp.sum(whole), F32)
    for send in sends:
        send.wait_send()

    @pl.loop(0, count)
    def _(k):
        @pl.loop(0, chips - 1)
        def _(s):
            for way in range(2):
                hop(k, way, s).wait_send()

    for j in range(2):
        swap(jnp.int32(count - 2 + j)).wait_send()


SOURCES = ((0, 4, True), (1, 2, False), (1, 3, False), (5, 7, True), (6, 8, False), (6, 9, False))
A0, DY0 = 6, 7


def summed(n, arrays, weights):
    tokens, d = arrays[1].shape
    ff = arrays[0].shape[1]
    r, chips, count, width = d // n, n // 2, len(SOURCES), ff // 6
    dma = pltpu.SemaphoreType.DMA
    like, any_spec, vmem_spec = jax.ShapeDtypeStruct, pl.BlockSpec(memory_space=ANY), pl.BlockSpec(memory_space=VMEM)
    operands = (*arrays, *weights)
    return pl.pallas_call(
        functools.partial(sum_kernel, n, len(operands)),
        out_shape=(like((count, r, ff), BF16), like((8, 128), F32), like((tokens, ff), BF16), like((tokens, ff), BF16)),
        in_specs=[any_spec] * len(operands),
        out_specs=(vmem_spec, vmem_spec, any_spec, any_spec),
        scratch_shapes=[
            VMEM((2, tokens, d), BF16),
            VMEM((2, tokens, d), BF16),
            VMEM((d, width), BF16),
            VMEM((d, width), BF16),
            VMEM((width, d), BF16),
            VMEM((6, chips, r, ff), BF16),
            VMEM((count, chips, r, ff), BF16),
            VMEM((count, 2, chips, r, ff // 2), BF16),
            VMEM((r, ff // 2), F32),
            VMEM((n, 8, 128), F32),
            dma((2, 2)),
            dma((7,)),
            dma((count,)),
            dma((count,)),
            dma((count, 2, chips - 1)),
            dma((count, 2, chips - 1)),
            dma((n,)),
            dma((n,)),
        ],
        compiler_params=pltpu.CompilerParams(collective_id=0, has_side_effects=True, vmem_limit_bytes=VMEM_BYTES),
        name="gradient_sum",
    )(*operands)


WEIGHTS = ((2, 1), (0, 1), (1, 1), (2, 0), (0, 0), (1, 0))


def pieces(k, array, block):
    name, layer = WEIGHTS[k]
    if name < 2:
        return [(array.at[layer], block)]
    tiles, width = array.shape[-3], array.shape[-1]
    lead = (slice(None),) * (len(array.shape) - 4)
    return [(array.at[(layer, *lead, q)], block.at[(*lead, slice(None), pl.ds(q * width, width))]) for q in range(tiles)]


def own_pieces(k, array, block, me):
    name, layer = WEIGHTS[k]
    if name < 2:
        return [(array.at[layer, me], block)]
    tiles, width = array.shape[-3], array.shape[-1]
    return [(array.at[layer, me, q], block.at[:, pl.ds(q * width, width)]) for q in range(tiles)]


def gather_kernel(n, g_ref, total_ref, *refs):
    w_in, m_in, v_in = (refs[i : i + 3] for i in range(0, 9, 3))
    count, r, ff = g_ref.shape
    w_out = refs[9 : 9 + count]
    m_out, v_out, w_buf, m_buf, v_buf, load_sem, store_sem, ring_send, ring_recv, pair_send, pair_recv = refs[9 + count :]
    half, chunk, chips = ff // 2, ff // 4, n // 2
    me = lax.axis_index("dp")
    z, c = lax.div(me, 2), lax.rem(me, 2)
    partner = 2 * z + 1 - c
    right = 2 * lax.rem(z + 1, chips) + c
    left = 2 * lax.rem(z + chips - 1, chips) + c
    onward = (right, left)

    def loads(k):
        name = WEIGHTS[k][0]
        parts = own_pieces(k, w_in[name], w_buf.at[k], me) + pieces(k, m_in[name], m_buf.at[k]) + pieces(k, v_in[name], v_buf.at[k])
        return [pltpu.make_async_copy(src, dst, load_sem.at[k, i]) for i, (src, dst) in enumerate(parts)]

    def stores(k):
        return (
            pltpu.make_async_copy(w_buf.at[k], w_out[k].at[me], store_sem.at[k, 0]),
            pltpu.make_async_copy(m_buf.at[k], m_out.at[k], store_sem.at[k, 1]),
            pltpu.make_async_copy(v_buf.at[k], v_out.at[k], store_sem.at[k, 2]),
        )

    def came(way, s):
        return lax.rem(z + chips - s, chips) if way == 0 else lax.rem(z + s, chips)

    def part(k, way, s):
        return w_out[k].at[2 * came(way, s) + c, :, pl.ds(way * half, half)]

    def hop(k, way, s, source=None):
        ref = part(k, way, s)
        return remote(ref if source is None else source, ref, ring_send.at[k, way, s], ring_recv.at[k, way, s], onward[way])

    def across(k, way, s, source=None):
        ref = part(k, way, s)
        return remote(ref if source is None else source, ref, pair_send.at[k, way, s], pair_recv.at[k, way, s], partner)

    enter((partner, left, right))
    for k in range(count):
        for copy in loads(k):
            copy.start()
    factor = jnp.minimum(1.0, 0.5 * lax.rsqrt(total_ref[0:1, 0:1] * (1.0 / (count * r * ff * n)) + 1e-30))

    for k in range(count):
        for copy in loads(k):
            copy.wait()

        @pl.loop(0, ff // chunk)
        def _(q):
            cols = pl.ds(pl.multiple_of(q * chunk, chunk), chunk)
            g = g_ref[k, :, cols].astype(F32) * factor
            m = 0.9 * m_buf[k, :, cols] + 0.1 * g
            v = 0.95 * v_buf[k, :, cols] + 0.05 * g * g
            w = w_buf[k, :, cols].astype(F32)
            step = m * lax.rsqrt(v + 1e-8) + 0.1 * w
            m_buf[k, :, cols] = m
            v_buf[k, :, cols] = v
            w_buf[k, :, cols] = (w - 0.02 * step).astype(BF16)

        if k == 0:
            meet(3)
        for way in range(2):
            own = w_buf.at[k, :, pl.ds(way * half, half)]
            hop(k, way, 0, own).start()
            across(k, way, 0, own).start()
        for copy in stores(k):
            copy.start()

    @pl.loop(1, chips)
    def _(s):
        for k in range(count):
            for way in range(2):
                hop(k, way, s - 1).wait_recv()

                @pl.when(s < chips - 1)
                def _():
                    hop(k, way, s).start()

                across(k, way, s).start()

    for k in range(count):
        for copy in stores(k):
            copy.wait()

        @pl.loop(0, chips)
        def _(s):
            for way in range(2):
                across(k, way, s).wait()

                @pl.when(s < chips - 1)
                def _():
                    hop(k, way, s).wait_send()


def stepped(n, g, total, w, m, v):
    count, r, ff = g.shape
    layers, d = w[0].shape[:2]
    chips, tiles = n // 2, ff // d
    dma = pltpu.SemaphoreType.DMA
    any_spec, vmem_spec = pl.BlockSpec(memory_space=ANY), pl.BlockSpec(memory_space=VMEM)
    row = (layers, r, ff), (layers, r, ff), (layers, tiles, r, d)
    whole = (layers, n, r, ff), (layers, n, r, ff), (layers, n, tiles, r, d)
    w = [t.reshape(s) for t, s in zip(w, whole, strict=True)]
    m, v = ([t.reshape(s) for t, s in zip(ts, row, strict=True)] for ts in (m, v))
    m, v = ([pltpu.with_memory_space_constraint(t, HBM) for t in ts] for ts in (m, v))
    held = pl.pallas_call(
        functools.partial(gather_kernel, n),
        out_shape=(*[VMEM((n, r, ff), BF16)] * count, *[jax.ShapeDtypeStruct((count, r, ff), F32)] * 2),
        in_specs=[vmem_spec] * 2 + [any_spec] * 9,
        out_specs=(any_spec,) * (count + 2),
        scratch_shapes=[
            *[VMEM((count, r, ff), t) for t in (BF16, F32, F32)],
            dma((count, 3 * tiles)),
            dma((count, 3)),
            *[dma((count, 2, chips - 1)) for _ in range(2)],
            *[dma((count, 2, chips)) for _ in range(2)],
        ],
        compiler_params=pltpu.CompilerParams(collective_id=1, has_side_effects=True, vmem_limit_bytes=27 * 1024 * 1024),
        name="step_and_gather",
    )(g, total, *w, *m, *v)

    def write_out(*refs):
        w_held, (m_held, v_held, *outs, sem) = refs[:count], refs[count:]
        parts = [
            pair
            for k, (name, _) in enumerate(WEIGHTS)
            for out, block in ((outs[name], w_held[k]), (outs[3 + name], m_held.at[k]), (outs[6 + name], v_held.at[k]))
            for pair in pieces(k, out, block)
        ]
        copies = [pltpu.make_async_copy(block, out, sem.at[i]) for i, (out, block) in enumerate(parts)]
        for copy in copies:
            copy.start()
        for copy in copies:
            copy.wait()

    outs = pl.pallas_call(
        write_out,
        out_shape=tuple(jax.ShapeDtypeStruct(t.shape, t.dtype) for t in (*w, *m, *v)),
        in_specs=[any_spec] * (count + 2),
        out_specs=(any_spec,) * 9,
        scratch_shapes=[dma((3 * count * tiles,))],
        compiler_params=pltpu.CompilerParams(vmem_limit_bytes=1024 * 1024),
        name="write_out",
    )(*held)
    rows = (layers, d, ff), (layers, d, ff), (layers, ff, d)
    blocks = (layers, r, ff), (layers, r, ff), (layers, tiles * r, d)
    return [t.reshape(s) for t, s in zip(outs, (*rows, *blocks, *blocks), strict=True)]


def normed(h):
    wide = h.astype(F32)
    scale = lax.rsqrt(jnp.mean(wide**2, -1, keepdims=True) + 1e-6)
    return (wide * scale).astype(BF16)


def back_through_norm(h, da):
    wide, g = h.astype(F32), da.astype(F32)
    mean = jnp.mean(wide**2, -1, keepdims=True) + 1e-6
    scale = lax.rsqrt(mean)
    inner = jnp.mean(g * wide, -1, keepdims=True)
    return (scale * g - wide * (inner * scale / mean)).astype(BF16)


def back_through_product(gate, up, s, dhid):
    p = dhid.astype(BF16).astype(F32)
    return (p * up * (s * (1 + gate * (1 - s)))).astype(BF16), (p * (gate * s)).astype(BF16)


def dot(a, b):
    return jnp.dot(a, b, preferred_element_type=F32)


def dot_t(a, b):
    return lax.dot_general(a, b, (((1,), (1,)), ((), ())), preferred_element_type=F32)


def forward_kernel(chunks, x_ref, wg_ref, wu_ref, wd_ref, a_ref, hid_ref, h_ref, acc):
    i = pl.program_id(0)
    size = x_ref.shape[0] // chunks

    @pl.when(i == 0)
    def _():
        a_ref[...] = normed(x_ref[...])
        acc[...] = jnp.zeros_like(acc)

    for q in range(chunks):
        rows = slice(q * size, (q + 1) * size)
        gate, up = dot(a_ref[rows], wg_ref[...]), dot(a_ref[rows], wu_ref[...])
        hid = (gate * jax.nn.sigmoid(gate) * up).astype(BF16)
        hid_ref[rows] = hid
        acc[rows] += dot(hid, wd_ref[...])

    @pl.when(i == pl.num_programs(0) - 1)
    def _():
        h_ref[...] = x_ref[...] + acc[...].astype(BF16)


def turn_kernel(chunks, h_ref, dy_ref, wg_ref, wu_ref, wd_ref, a_ref, hid_ref, dgate_ref, dup_ref, dh_ref, acc_g, acc_u):
    i = pl.program_id(0)
    size = h_ref.shape[0] // chunks

    @pl.when(i == 0)
    def _():
        a_ref[...] = normed(h_ref[...])
        acc_g[...] = jnp.zeros_like(acc_g)
        acc_u[...] = jnp.zeros_like(acc_u)

    for q in range(chunks):
        rows = slice(q * size, (q + 1) * size)
        gate, up = dot(a_ref[rows], wg_ref[...]), dot(a_ref[rows], wu_ref[...])
        dhid = dot_t(dy_ref[rows], wd_ref[...])
        s = jax.nn.sigmoid(gate)
        hid_ref[rows] = (gate * s * up).astype(BF16)
        dgate, dup = back_through_product(gate, up, s, dhid)
        dgate_ref[rows], dup_ref[rows] = dgate, dup
        acc_g[rows] += dot_t(dgate, wg_ref[...])
        acc_u[rows] += dot_t(dup, wu_ref[...])

    @pl.when(i == pl.num_programs(0) - 1)
    def _():
        da = acc_g[...].astype(BF16) + acc_u[...].astype(BF16)
        dh_ref[...] = dy_ref[...] + back_through_norm(h_ref[...], da)


def operands(x, dy, w_gate, w_up, w_down):
    (tokens, d), ff = x.shape, w_gate.shape[2]
    tile, chunks = ff // 6, 2
    grid = (ff // tile,)
    like = jax.ShapeDtypeStruct
    state, states = pl.BlockSpec((tokens, d), lambda i: (0, 0)), like((tokens, d), BF16)
    hidden, hiddens = pl.BlockSpec((tokens, tile), lambda i: (0, i)), like((tokens, ff), BF16)

    def into(layer):
        return pl.BlockSpec((None, d, tile), lambda i: (layer, 0, i))

    def out_of(layer):
        return pl.BlockSpec((None, tile, d), lambda i: (layer, i, 0))

    acc = VMEM((tokens, d), F32)
    params = pltpu.CompilerParams(vmem_limit_bytes=56 * 1024 * 1024, dimension_semantics=("arbitrary",))
    a0, hid0, h1 = pl.pallas_call(
        functools.partial(forward_kernel, chunks),
        grid=grid,
        out_shape=(states, hiddens, states),
        in_specs=[state, into(0), into(0), out_of(0)],
        out_specs=(state, hidden, state),
        scratch_shapes=[acc],
        compiler_params=params,
        name="first_forward",
    )(x, w_gate, w_up, w_down)
    a1, hid1, dgate1, dup1, dy0 = pl.pallas_call(
        functools.partial(turn_kernel, chunks),
        grid=grid,
        out_shape=(states, hiddens, hiddens, hiddens, states),
        in_specs=[state, state, into(1), into(1), out_of(1)],
        out_specs=(state, hidden, hidden, hidden, state),
        scratch_shapes=[acc, acc],
        compiler_params=params,
        name="last_layer",
    )(h1, dy, w_gate, w_up, w_down)
    return hid1, a1, dgate1, dup1, dy, hid0, a0, dy0


def solution(mesh):
    n = mesh.shape["dp"]

    def device(x, dy, *arrays):
        w, m, v = (arrays[i : i + 3] for i in (0, 3, 6))
        g, total, *_ = summed(n, operands(x[0], dy[0], *w), w)
        return tuple(stepped(n, g, total, w, m, v))

    whole, rows = P(None, None, None), P(None, "dp", None)
    tokens = P(("rep", "dp"), None, None)
    return jax.shard_map(
        device,
        mesh=mesh,
        in_specs=(tokens, tokens, *[whole] * 3, *[rows] * 6),
        out_specs=(*[P("rep", None, None)] * 3, *[P("rep", "dp", None)] * 6),
        check_vma=False,
    )
```

```python
import functools

import jax
import jax.numpy as jnp
from jax import lax
from jax.experimental import pallas as pl
from jax.experimental.pallas import tpu as pltpu
from jax.sharding import PartitionSpec as P

F32, BF16 = jnp.float32, jnp.bfloat16
ANY, HBM, VMEM = pl.ANY, pltpu.HBM, pltpu.VMEM
MESH = pl.DeviceIdType.MESH
VMEM_BYTES = 64 * 1024 * 1024 - 65536


def remote(src, dst, send, recv, to):
    return pltpu.make_async_remote_copy(
        src_ref=src, dst_ref=dst, send_sem=send, recv_sem=recv, device_id={"dp": to}, device_id_type=MESH
    )


def enter(peers):
    for peer in peers:
        pl.semaphore_signal(pltpu.get_barrier_semaphore(), inc=1, device_id={"dp": peer}, device_id_type=MESH)


def meet(count):
    pl.semaphore_wait(pltpu.get_barrier_semaphore(), count)


def sum_kernel(n, inputs_count, *refs):
    hid, a, dgate1, dup1, dy, dh, wg, wu, wd = refs[:inputs_count]
    g_ref, total_ref, dgate, dup = refs[inputs_count : inputs_count + 4]
    (a_buf, b_buf, wg_buf, wu_buf, wd_buf, mine, theirs, ring, squares, slots, *sems) = refs[inputs_count + 4 :]
    load_sem, back_sem, swap_send, swap_recv, ring_send, ring_recv, all_send, all_recv = sems
    inputs = [hid.at[1], a.at[1], dgate1, dup1, dy, hid.at[0], a.at[0], dh, dgate, dup]
    d = a_buf.shape[2]
    r, ff = mine.shape[2:]
    half, tiles, chips = ff // 2, ff // d, n // 2
    width = wg_buf.shape[1]
    backs = ff // width
    late = backs - (chips - 1 - tiles)
    shift = 2 * late - 1
    count = ring.shape[0]
    pairs = count // 2
    me = lax.axis_index("dp")
    z, c = lax.div(me, 2), lax.rem(me, 2)
    partner = 2 * z + 1 - c
    right = 2 * lax.rem(z + 1, chips) + c
    left = 2 * lax.rem(z + chips - 1, chips) + c
    onward = (right, left)

    def loads(k, t, slot):
        a, b, a_moves = sources_of[k]
        moving = pl.ds(pl.multiple_of(t * d, d), d)
        whole = pl.ds(0, d)
        return (
            pltpu.make_async_copy(a.at[:, moving if a_moves else whole], a_buf.at[slot], load_sem.at[slot, 0]),
            pltpu.make_async_copy(b.at[:, whole if a_moves else moving], b_buf.at[slot], load_sem.at[slot, 1]),
        )

    sources_of = [(inputs[ia], inputs[ib], moves) for ia, ib, moves in SOURCES]

    def back_loads(u):
        at = pl.ds(pl.multiple_of(u * width, width), width)
        return (
            pltpu.make_async_copy(wg.at[0, :, at], wg_buf, back_sem.at[0]),
            pltpu.make_async_copy(wu.at[0, :, at], wu_buf, back_sem.at[1]),
            pltpu.make_async_copy(wd.at[0, at], wd_buf, back_sem.at[2]),
        )

    def back_states():
        return (
            pltpu.make_async_copy(inputs[A0], a_buf.at[0], back_sem.at[3]),
            pltpu.make_async_copy(inputs[DY0], b_buf.at[0], back_sem.at[4]),
        )

    def back_stores(u):
        at = pl.ds(pl.multiple_of(u * width, width), width)
        return (
            pltpu.make_async_copy(a_buf.at[1, :, pl.ds(0, width)], dgate.at[:, at], back_sem.at[5]),
            pltpu.make_async_copy(b_buf.at[1, :, pl.ds(0, width)], dup.at[:, at], back_sem.at[6]),
        )

    def back(u):
        @pl.when(u == 0)
        def _():
            for copy in back_states():
                copy.wait()

        @pl.when(u > 0)
        def _():
            for copy in back_stores(u - 1):
                copy.wait()

        for copy in back_loads(u):
            copy.wait()
        size = a_buf.shape[1] // 4
        for q in range(4):
            rows = slice(q * size, (q + 1) * size)
            gate, up = dot(a_buf[0, rows], wg_buf[...]), dot(a_buf[0, rows], wu_buf[...])
            dhid = dot_t(b_buf[0, rows], wd_buf[...])
            a_buf[1, rows, :width], b_buf[1, rows, :width] = back_through_product(gate, up, jax.nn.sigmoid(gate), dhid)
        for copy in back_stores(u):
            copy.start()

        @pl.when(u + 1 < backs)
        def _():
            for copy in back_loads(u + 1):
                copy.start()

        @pl.when(u + 1 == backs)
        def _():
            for copy in back_stores(u):
                copy.wait()
            start_load(jnp.int32(2 * tiles * 2))

    def start_load(index):
        for k in range(count):

            @pl.when(lax.div(index, tiles) == k)
            def _():
                for copy in loads(k, lax.rem(index, tiles), lax.rem(index, 2)):
                    copy.start()

    def swap(k):
        return remote(mine.at[4 + lax.rem(k, 2)], theirs.at[k], swap_send.at[k], swap_recv.at[k], partner)

    def hop(k, way, s):
        return remote(ring.at[k, way, s], ring.at[k, way, s + 1], ring_send.at[k, way, s], ring_recv.at[k, way, s], onward[way])

    def tile(index, swaps=True):
        k, t, slot = lax.div(index, tiles), lax.rem(index, tiles), lax.rem(index, 2)

        @pl.when(jnp.logical_and(index + 1 < count * tiles, index + 1 != 4 * tiles))
        def _():
            start_load(index + 1)

        @pl.when(index + 1 == 4 * tiles)
        def _():
            for copy in back_loads(jnp.int32(0)):
                copy.start()

        @pl.when(jnp.logical_and(t == 0, k >= 2))
        def _():
            swap(k - 2).wait_send()

        for copy in loads(0, 0, slot):
            copy.wait()
        down = 1 - lax.div(lax.rem(k, 3) + 1, 2)
        for part in range(2):
            cols = d // 2
            out = lax.dot_general(
                a_buf[slot, :, part * cols : (part + 1) * cols], b_buf[slot], (((0,), (0,)), ((), ())), preferred_element_type=F32
            ).astype(BF16)
            for i in range(cols // r):
                group = part * (cols // r) + i
                device = down * (t * (n // tiles) + group // tiles) + (1 - down) * group
                at = down * ((group % tiles) * d) + (1 - down) * (t * d)
                same = 1 - lax.rem(lax.rem(device, 2) + c, 2)
                buf = same * lax.rem(k, 4) + (1 - same) * (4 + lax.rem(k, 2))
                mine[buf, lax.div(device, 2), :, pl.ds(pl.multiple_of(at, d), d)] = out[i * r : (i + 1) * r]

        if swaps:

            @pl.when(t == tiles - 1)
            def _():
                swap(k).start()

    def term(k, way, chip):
        cols = slice(way * half, (way + 1) * half)
        return mine[lax.rem(k, 4), chip, :, cols].astype(F32) + theirs[k, chip, :, cols].astype(F32)

    def meant_for(way, s):
        return lax.rem(z + chips - 1 - s, chips) if way == 0 else lax.rem(z + 1 + s, chips)

    def first(k):
        swap(k).wait_recv()
        for way in range(2):
            ring[k, way, 0] = term(k, way, meant_for(way, 0)).astype(BF16)
            hop(k, way, 0).start()

    def middle(k, s):
        for way in range(2):
            hop(k, way, s - 1).wait_recv()
            ring[k, way, s] = (term(k, way, meant_for(way, s)) + ring[k, way, s].astype(F32)).astype(BF16)
            hop(k, way, s).start()

    def last(k):
        for way in range(2):
            hop(k, way, chips - 2).wait_recv()
            g = (term(k, way, z) + ring[k, way, chips - 1].astype(F32)).astype(BF16)
            g_ref[k, :, way * half : (way + 1) * half] = g
            squares[...] += g.astype(F32) * g.astype(F32)

    enter([lax.rem(me + o, n) for o in range(1, n)])
    start_load(0)
    squares[...] = jnp.zeros_like(squares)

    @pl.loop(0, tiles)
    def _(index):
        tile(index, swaps=False)

    meet(n - 1)
    swap(jnp.int32(0)).start()

    @pl.loop(0, pairs + 1)
    def _(ii):
        @pl.loop(0, chips - 1)
        def _(s):
            for j in range(2):
                k = 2 * (ii - 1) + j

                @pl.when(jnp.logical_and(ii > 0, jnp.logical_and(s == 0, k > 0)))
                def _():
                    first(k)

                @pl.when(jnp.logical_and(ii > 0, s > 0))
                def _():
                    middle(k, s)

                @pl.when(jnp.logical_and(ii > 1, s == 0))
                def _():
                    last(k - 2)

                if j == 0:

                    @pl.when(jnp.logical_and(ii == 0, s == tiles - 1))
                    def _():
                        first(jnp.int32(0))

                place = 2 * s + j - shift * lax.div(ii, 2)

                @pl.when(jnp.logical_and(ii < pairs, jnp.logical_and(place >= tiles * (1 - lax.div(ii + 2, 3)), place < 2 * tiles)))
                def _():
                    tile(2 * tiles * ii + place)

                if j == 0:

                    @pl.when(jnp.logical_and(ii == 1, s == tiles))
                    def _():
                        for copy in back_states():
                            copy.start()

                if j == 0:
                    due, u = jnp.logical_and(ii == 2, s == late - 1), jnp.int32(backs - 1)
                else:
                    due = jnp.logical_or(jnp.logical_and(ii == 1, s >= tiles), jnp.logical_and(ii == 2, s < late - 1))
                    u = s - tiles + (ii - 1) * (chips - 1)

                @pl.when(due)
                def _():
                    back(u)

    for j in range(2):
        last(jnp.int32(count - 2 + j))

    whole = squares[0:8, 0:128]
    for i in range(r // 8):
        for q in range(half // 128):
            if i or q:
                whole = whole + squares[i * 8 : (i + 1) * 8, q * 128 : (q + 1) * 128]
    slots[0] = whole
    sends = [remote(slots.at[0], slots.at[o], all_send.at[o], all_recv.at[o], lax.rem(me + o, n)) for o in range(1, n)]
    for send in sends:
        send.start()
    for send in sends:
        send.wait_recv()
    whole = slots[0]
    for o in range(1, n):
        whole = whole + slots[o]
    total_ref[...] = jnp.full(total_ref.shape, jnp.sum(whole), F32)
    for send in sends:
        send.wait_send()

    @pl.loop(0, count)
    def _(k):
        @pl.loop(0, chips - 1)
        def _(s):
            for way in range(2):
                hop(k, way, s).wait_send()

    for j in range(2):
        swap(jnp.int32(count - 2 + j)).wait_send()


SOURCES = ((0, 4, True), (1, 2, False), (1, 3, False), (5, 7, True), (6, 8, False), (6, 9, False))
A0, DY0 = 6, 7


def summed(n, arrays, weights):
    tokens, d = arrays[1].shape[1:]
    ff = arrays[0].shape[2]
    r, chips, count, width = d // n, n // 2, len(SOURCES), ff // 6
    dma = pltpu.SemaphoreType.DMA
    like, any_spec, vmem_spec = jax.ShapeDtypeStruct, pl.BlockSpec(memory_space=ANY), pl.BlockSpec(memory_space=VMEM)
    operands = (*arrays, *weights)
    return pl.pallas_call(
        functools.partial(sum_kernel, n, len(operands)),
        out_shape=(like((count, r, ff), BF16), like((8, 128), F32), like((tokens, ff), BF16), like((tokens, ff), BF16)),
        in_specs=[any_spec] * len(operands),
        out_specs=(vmem_spec, vmem_spec, any_spec, any_spec),
        scratch_shapes=[
            VMEM((2, tokens, d), BF16),
            VMEM((2, tokens, d), BF16),
            VMEM((d, width), BF16),
            VMEM((d, width), BF16),
            VMEM((width, d), BF16),
            VMEM((6, chips, r, ff), BF16),
            VMEM((count, chips, r, ff), BF16),
            VMEM((count, 2, chips, r, ff // 2), BF16),
            VMEM((r, ff // 2), F32),
            VMEM((n, 8, 128), F32),
            dma((2, 2)),
            dma((7,)),
            dma((count,)),
            dma((count,)),
            dma((count, 2, chips - 1)),
            dma((count, 2, chips - 1)),
            dma((n,)),
            dma((n,)),
        ],
        compiler_params=pltpu.CompilerParams(collective_id=0, has_side_effects=True, vmem_limit_bytes=VMEM_BYTES),
        name="gradient_sum",
    )(*operands)


WEIGHTS = ((2, 1), (0, 1), (1, 1), (2, 0), (0, 0), (1, 0))


def pieces(k, array, block):
    name, layer = WEIGHTS[k]
    if name < 2:
        return [(array.at[layer], block)]
    tiles, width = array.shape[-3], array.shape[-1]
    lead = (slice(None),) * (len(array.shape) - 4)
    return [(array.at[(layer, *lead, q)], block.at[(*lead, slice(None), pl.ds(q * width, width))]) for q in range(tiles)]


def own_pieces(k, array, block, me):
    name, layer = WEIGHTS[k]
    if name < 2:
        return [(array.at[layer, me], block)]
    tiles, width = array.shape[-3], array.shape[-1]
    return [(array.at[layer, me, q], block.at[:, pl.ds(q * width, width)]) for q in range(tiles)]


def gather_kernel(n, g_ref, total_ref, *refs):
    w_in, m_in, v_in = (refs[i : i + 3] for i in range(0, 9, 3))
    count, r, ff = g_ref.shape
    w_out = refs[9 : 9 + count]
    m_out, v_out, w_buf, m_buf, v_buf, load_sem, store_sem, ring_send, ring_recv, pair_send, pair_recv = refs[9 + count :]
    half, chunk, chips = ff // 2, ff // 4, n // 2
    me = lax.axis_index("dp")
    z, c = lax.div(me, 2), lax.rem(me, 2)
    partner = 2 * z + 1 - c
    right = 2 * lax.rem(z + 1, chips) + c
    left = 2 * lax.rem(z + chips - 1, chips) + c
    onward = (right, left)

    def loads(k):
        name = WEIGHTS[k][0]
        parts = own_pieces(k, w_in[name], w_buf.at[k], me) + pieces(k, m_in[name], m_buf.at[k]) + pieces(k, v_in[name], v_buf.at[k])
        return [pltpu.make_async_copy(src, dst, load_sem.at[k, i]) for i, (src, dst) in enumerate(parts)]

    def stores(k):
        return (
            pltpu.make_async_copy(w_buf.at[k], w_out[k].at[me], store_sem.at[k, 0]),
            pltpu.make_async_copy(m_buf.at[k], m_out.at[k], store_sem.at[k, 1]),
            pltpu.make_async_copy(v_buf.at[k], v_out.at[k], store_sem.at[k, 2]),
        )

    def came(way, s):
        return lax.rem(z + chips - s, chips) if way == 0 else lax.rem(z + s, chips)

    def part(k, way, s):
        return w_out[k].at[2 * came(way, s) + c, :, pl.ds(way * half, half)]

    def hop(k, way, s, source=None):
        ref = part(k, way, s)
        return remote(ref if source is None else source, ref, ring_send.at[k, way, s], ring_recv.at[k, way, s], onward[way])

    def across(k, way, s, source=None):
        ref = part(k, way, s)
        return remote(ref if source is None else source, ref, pair_send.at[k, way, s], pair_recv.at[k, way, s], partner)

    enter((partner, left, right))
    for k in range(count):
        for copy in loads(k):
            copy.start()
    factor = jnp.minimum(1.0, 0.5 * lax.rsqrt(total_ref[0:1, 0:1] * (1.0 / (count * r * ff * n)) + 1e-30))

    for k in range(count):
        for copy in loads(k):
            copy.wait()

        @pl.loop(0, ff // chunk)
        def _(q):
            cols = pl.ds(pl.multiple_of(q * chunk, chunk), chunk)
            g = g_ref[k, :, cols].astype(F32) * factor
            m = 0.9 * m_buf[k, :, cols] + 0.1 * g
            v = 0.95 * v_buf[k, :, cols] + 0.05 * g * g
            w = w_buf[k, :, cols].astype(F32)
            step = m * lax.rsqrt(v + 1e-8) + 0.1 * w
            m_buf[k, :, cols] = m
            v_buf[k, :, cols] = v
            w_buf[k, :, cols] = (w - 0.02 * step).astype(BF16)

        if k == 0:
            meet(3)
        for way in range(2):
            own = w_buf.at[k, :, pl.ds(way * half, half)]
            hop(k, way, 0, own).start()
            across(k, way, 0, own).start()
        for copy in stores(k):
            copy.start()

    @pl.loop(1, chips)
    def _(s):
        for k in range(count):
            for way in range(2):
                hop(k, way, s - 1).wait_recv()

                @pl.when(s < chips - 1)
                def _():
                    hop(k, way, s).start()

                across(k, way, s).start()

    for k in range(count):
        for copy in stores(k):
            copy.wait()

        @pl.loop(0, chips)
        def _(s):
            for way in range(2):
                across(k, way, s).wait()

                @pl.when(s < chips - 1)
                def _():
                    hop(k, way, s).wait_send()


def stepped(n, g, total, w, m, v):
    count, r, ff = g.shape
    layers, d = w[0].shape[:2]
    chips, tiles = n // 2, ff // d
    dma = pltpu.SemaphoreType.DMA
    any_spec, vmem_spec = pl.BlockSpec(memory_space=ANY), pl.BlockSpec(memory_space=VMEM)
    row = (layers, r, ff), (layers, r, ff), (layers, tiles, r, d)
    whole = (layers, n, r, ff), (layers, n, r, ff), (layers, n, tiles, r, d)
    w = [t.reshape(s) for t, s in zip(w, whole, strict=True)]
    m, v = ([t.reshape(s) for t, s in zip(ts, row, strict=True)] for ts in (m, v))
    m, v = ([pltpu.with_memory_space_constraint(t, HBM) for t in ts] for ts in (m, v))
    held = pl.pallas_call(
        functools.partial(gather_kernel, n),
        out_shape=(*[VMEM((n, r, ff), BF16)] * count, *[jax.ShapeDtypeStruct((count, r, ff), F32)] * 2),
        in_specs=[vmem_spec] * 2 + [any_spec] * 9,
        out_specs=(any_spec,) * (count + 2),
        scratch_shapes=[
            *[VMEM((count, r, ff), t) for t in (BF16, F32, F32)],
            dma((count, 3 * tiles)),
            dma((count, 3)),
            *[dma((count, 2, chips - 1)) for _ in range(2)],
            *[dma((count, 2, chips)) for _ in range(2)],
        ],
        compiler_params=pltpu.CompilerParams(collective_id=1, has_side_effects=True, vmem_limit_bytes=27 * 1024 * 1024),
        name="step_and_gather",
    )(g, total, *w, *m, *v)

    def write_out(*refs):
        w_held, (m_held, v_held, *outs, sem) = refs[:count], refs[count:]
        parts = [
            pair
            for k, (name, _) in enumerate(WEIGHTS)
            for out, block in ((outs[name], w_held[k]), (outs[3 + name], m_held.at[k]), (outs[6 + name], v_held.at[k]))
            for pair in pieces(k, out, block)
        ]
        copies = [pltpu.make_async_copy(block, out, sem.at[i]) for i, (out, block) in enumerate(parts)]
        for copy in copies:
            copy.start()
        for copy in copies:
            copy.wait()

    outs = pl.pallas_call(
        write_out,
        out_shape=tuple(jax.ShapeDtypeStruct(t.shape, t.dtype) for t in (*w, *m, *v)),
        in_specs=[any_spec] * (count + 2),
        out_specs=(any_spec,) * 9,
        scratch_shapes=[dma((3 * count * tiles,))],
        compiler_params=pltpu.CompilerParams(vmem_limit_bytes=1024 * 1024),
        name="write_out",
    )(*held)
    rows = (layers, d, ff), (layers, d, ff), (layers, ff, d)
    blocks = (layers, r, ff), (layers, r, ff), (layers, tiles * r, d)
    return [t.reshape(s) for t, s in zip(outs, (*rows, *blocks, *blocks), strict=True)]


def normed(h):
    wide = h.astype(F32)
    scale = lax.rsqrt(jnp.mean(wide**2, -1, keepdims=True) + 1e-6)
    return (wide * scale).astype(BF16)


def back_through_norm(h, da):
    wide, g = h.astype(F32), da.astype(F32)
    mean = jnp.mean(wide**2, -1, keepdims=True) + 1e-6
    scale = lax.rsqrt(mean)
    inner = jnp.mean(g * wide, -1, keepdims=True)
    return (scale * g - wide * (inner * scale / mean)).astype(BF16)


def back_through_product(gate, up, s, dhid):
    p = dhid.astype(BF16).astype(F32)
    return (p * up * (s * (1 + gate * (1 - s)))).astype(BF16), (p * (gate * s)).astype(BF16)


def dot(a, b):
    return jnp.dot(a, b, preferred_element_type=F32)


def dot_t(a, b):
    return lax.dot_general(a, b, (((1,), (1,)), ((), ())), preferred_element_type=F32)


def layers_kernel(chunks, x_ref, dy_ref, wg_ref, wu_ref, wd_ref, a_ref, hid_ref, dgate_ref, dup_ref, dh_ref, h, acc_g, acc_u):
    turn, i, end = pl.program_id(0) == 1, pl.program_id(1), pl.num_programs(1) - 1
    first = jnp.logical_not(turn)
    size = x_ref.shape[0] // chunks

    @pl.when(jnp.logical_and(first, i == 0))
    def _():
        a_ref[...] = normed(x_ref[...])
        acc_g[...] = jnp.zeros_like(acc_g)

    @pl.when(jnp.logical_and(turn, i == 0))
    def _():
        a_ref[...] = normed(h[...])
        acc_g[...] = jnp.zeros_like(acc_g)
        acc_u[...] = jnp.zeros_like(acc_u)

    @pl.when(first)
    def _():
        for q in range(chunks):
            rows = slice(q * size, (q + 1) * size)
            gate, up = dot(a_ref[rows], wg_ref[...]), dot(a_ref[rows], wu_ref[...])
            hid = (gate * jax.nn.sigmoid(gate) * up).astype(BF16)
            hid_ref[rows] = hid
            acc_g[rows] += dot(hid, wd_ref[...])

    @pl.when(turn)
    def _():
        for q in range(chunks):
            rows = slice(q * size, (q + 1) * size)
            gate, up = dot(a_ref[rows], wg_ref[...]), dot(a_ref[rows], wu_ref[...])
            dhid = dot_t(dy_ref[rows], wd_ref[...])
            s = jax.nn.sigmoid(gate)
            hid_ref[rows] = (gate * s * up).astype(BF16)
            dgate, dup = back_through_product(gate, up, s, dhid)
            dgate_ref[rows], dup_ref[rows] = dgate, dup
            acc_g[rows] += dot_t(dgate, wg_ref[...])
            acc_u[rows] += dot_t(dup, wu_ref[...])

    @pl.when(jnp.logical_and(first, i == end))
    def _():
        h[...] = x_ref[...] + acc_g[...].astype(BF16)

    @pl.when(jnp.logical_and(turn, i == end))
    def _():
        da = acc_g[...].astype(BF16) + acc_u[...].astype(BF16)
        dh_ref[...] = dy_ref[...] + back_through_norm(h[...], da)


def operands(x, dy, w_gate, w_up, w_down):
    (tokens, d), (layers, _, ff) = x.shape, w_gate.shape
    tile, chunks = ff // 6, 2
    like = jax.ShapeDtypeStruct
    state = pl.BlockSpec((tokens, d), lambda l, i: (0, 0))
    into = pl.BlockSpec((None, d, tile), lambda l, i: (l, 0, i))
    last = pl.BlockSpec((tokens, tile), lambda l, i: (0, l * i))
    a, hid, dgate, dup, dh = pl.pallas_call(
        functools.partial(layers_kernel, chunks),
        grid=(layers, ff // tile),
        out_shape=(
            like((layers, tokens, d), BF16),
            like((layers, tokens, ff), BF16),
            like((tokens, ff), BF16),
            like((tokens, ff), BF16),
            like((tokens, d), BF16),
        ),
        in_specs=[state, state, into, into, pl.BlockSpec((None, tile, d), lambda l, i: (l, i, 0))],
        out_specs=(
            pl.BlockSpec((None, tokens, d), lambda l, i: (l, 0, 0)),
            pl.BlockSpec((None, tokens, tile), lambda l, i: (l, 0, i)),
            last,
            last,
            state,
        ),
        scratch_shapes=[VMEM((tokens, d), BF16), VMEM((tokens, d), F32), VMEM((tokens, d), F32)],
        compiler_params=pltpu.CompilerParams(vmem_limit_bytes=58 * 1024 * 1024, dimension_semantics=("arbitrary", "arbitrary")),
        name="layers",
    )(x, dy, w_gate, w_up, w_down)
    return hid, a, dgate, dup, dy, dh


def solution(mesh):
    n = mesh.shape["dp"]

    def device(x, dy, *arrays):
        w, m, v = (arrays[i : i + 3] for i in (0, 3, 6))
        g, total, *_ = summed(n, operands(x[0], dy[0], *w), w)
        return tuple(stepped(n, g, total, w, m, v))

    whole, rows = P(None, None, None), P(None, "dp", None)
    tokens = P(("rep", "dp"), None, None)
    return jax.shard_map(
        device,
        mesh=mesh,
        in_specs=(tokens, tokens, *[whole] * 3, *[rows] * 6),
        out_specs=(*[P("rep", None, None)] * 3, *[P("rep", "dp", None)] * 6),
        check_vma=False,
    )
```

```python
import functools

import jax
import jax.numpy as jnp
from jax import lax
from jax.experimental import pallas as pl
from jax.experimental.pallas import tpu as pltpu
from jax.sharding import PartitionSpec as P

F32, BF16 = jnp.float32, jnp.bfloat16
ANY, HBM, VMEM = pl.ANY, pltpu.HBM, pltpu.VMEM
MESH = pl.DeviceIdType.MESH
VMEM_BYTES = 64 * 1024 * 1024 - 65536


def remote(src, dst, send, recv, to):
    return pltpu.make_async_remote_copy(
        src_ref=src, dst_ref=dst, send_sem=send, recv_sem=recv, device_id={"dp": to}, device_id_type=MESH
    )


def enter(peers):
    for peer in peers:
        pl.semaphore_signal(pltpu.get_barrier_semaphore(), inc=1, device_id={"dp": peer}, device_id_type=MESH)


def meet(count):
    pl.semaphore_wait(pltpu.get_barrier_semaphore(), count)


LANES = (0, 2, 1, 3)


def sum_kernel(n, inputs_count, *refs):
    hid, a, dgate1, dup1, dy, dh, wg, wu, wd = refs[:inputs_count]
    g_ref, total_ref, dgate, dup = refs[inputs_count : inputs_count + 4]
    (a_buf, b_buf, wg_buf, wu_buf, wd_buf, mine, theirs, ring, squares, slots, *sems) = refs[inputs_count + 4 :]
    load_sem, back_sem, swap_send, swap_recv, ring_send, ring_recv, all_send, all_recv = sems
    inputs = [hid.at[1], a.at[1], dgate1, dup1, dy, hid.at[0], a.at[0], dh, dgate, dup]
    d = a_buf.shape[2]
    r, ff = mine.shape[2:]
    quarter, tiles, chips = ff // 4, ff // d, n // 2
    width = wg_buf.shape[1]
    backs = ff // width
    late = backs - (chips - 1 - tiles)
    shift = 2 * late - 1
    count = ring.shape[0]
    pairs = count // 2
    me = lax.axis_index("dp")
    z, c = lax.div(me, 2), lax.rem(me, 2)
    partner = 2 * z + 1 - c
    right = 2 * lax.rem(z + 1, chips) + c
    left = 2 * lax.rem(z + chips - 1, chips) + c
    onward = (right, left)

    def loads(k, t, slot):
        a, b, a_moves = sources_of[k]
        moving = pl.ds(pl.multiple_of(t * d, d), d)
        whole = pl.ds(0, d)
        return (
            pltpu.make_async_copy(a.at[:, moving if a_moves else whole], a_buf.at[slot], load_sem.at[slot, 0]),
            pltpu.make_async_copy(b.at[:, whole if a_moves else moving], b_buf.at[slot], load_sem.at[slot, 1]),
        )

    sources_of = [(inputs[ia], inputs[ib], moves) for ia, ib, moves in SOURCES]

    def back_loads(u):
        at = pl.ds(pl.multiple_of(u * width, width), width)
        return (
            pltpu.make_async_copy(wg.at[0, :, at], wg_buf, back_sem.at[0]),
            pltpu.make_async_copy(wu.at[0, :, at], wu_buf, back_sem.at[1]),
            pltpu.make_async_copy(wd.at[0, at], wd_buf, back_sem.at[2]),
        )

    def back_states():
        return (
            pltpu.make_async_copy(inputs[A0], a_buf.at[0], back_sem.at[3]),
            pltpu.make_async_copy(inputs[DY0], b_buf.at[0], back_sem.at[4]),
        )

    def back_stores(u):
        at = pl.ds(pl.multiple_of(u * width, width), width)
        return (
            pltpu.make_async_copy(a_buf.at[1, :, pl.ds(0, width)], dgate.at[:, at], back_sem.at[5]),
            pltpu.make_async_copy(b_buf.at[1, :, pl.ds(0, width)], dup.at[:, at], back_sem.at[6]),
        )

    def back(u):
        @pl.when(u == 0)
        def _():
            for copy in back_states():
                copy.wait()

        @pl.when(u > 0)
        def _():
            for copy in back_stores(u - 1):
                copy.wait()

        for copy in back_loads(u):
            copy.wait()
        size = a_buf.shape[1] // 4
        for q in range(4):
            rows = slice(q * size, (q + 1) * size)
            gate, up = dot(a_buf[0, rows], wg_buf[...]), dot(a_buf[0, rows], wu_buf[...])
            dhid = dot_t(b_buf[0, rows], wd_buf[...])
            a_buf[1, rows, :width], b_buf[1, rows, :width] = back_through_product(gate, up, jax.nn.sigmoid(gate), dhid)
        for copy in back_stores(u):
            copy.start()

        @pl.when(u + 1 < backs)
        def _():
            for copy in back_loads(u + 1):
                copy.start()

        @pl.when(u + 1 == backs)
        def _():
            for copy in back_stores(u):
                copy.wait()
            start_load(jnp.int32(2 * tiles * 2))

    def start_load(index):
        for k in range(count):

            @pl.when(lax.div(index, tiles) == k)
            def _():
                for copy in loads(k, lax.rem(index, tiles), lax.rem(index, 2)):
                    copy.start()

    def swap(k):
        return remote(mine.at[4 + lax.rem(k, 2)], theirs.at[k], swap_send.at[k], swap_recv.at[k], partner)

    def hop(k, lane, s):
        to = onward[lane // 2]
        return remote(ring.at[k, lane, s], ring.at[k, lane, s + 1], ring_send.at[k, lane, s], ring_recv.at[k, lane, s], to)

    def tile(index, swaps=True):
        k, t, slot = lax.div(index, tiles), lax.rem(index, tiles), lax.rem(index, 2)

        @pl.when(jnp.logical_and(index + 1 < count * tiles, index + 1 != 4 * tiles))
        def _():
            start_load(index + 1)

        @pl.when(index + 1 == 4 * tiles)
        def _():
            for copy in back_loads(jnp.int32(0)):
                copy.start()

        @pl.when(jnp.logical_and(t == 0, k >= 2))
        def _():
            swap(k - 2).wait_send()

        for copy in loads(0, 0, slot):
            copy.wait()
        down = 1 - lax.div(lax.rem(k, 3) + 1, 2)
        for part in range(2):
            cols = d // 2
            out = lax.dot_general(
                a_buf[slot, :, part * cols : (part + 1) * cols], b_buf[slot], (((0,), (0,)), ((), ())), preferred_element_type=F32
            ).astype(BF16)
            for i in range(cols // r):
                group = part * (cols // r) + i
                device = down * (t * (n // tiles) + group // tiles) + (1 - down) * group
                at = down * ((group % tiles) * d) + (1 - down) * (t * d)
                same = 1 - lax.rem(lax.rem(device, 2) + c, 2)
                buf = same * lax.rem(k, 4) + (1 - same) * (4 + lax.rem(k, 2))
                mine[buf, lax.div(device, 2), :, pl.ds(pl.multiple_of(at, d), d)] = out[i * r : (i + 1) * r]

        if swaps:

            @pl.when(t == tiles - 1)
            def _():
                swap(k).start()

    def columns(lane):
        return slice(lane * quarter, (lane + 1) * quarter)

    def term(k, lane, chip):
        return mine[lax.rem(k, 4), chip, :, columns(lane)].astype(F32) + theirs[k, chip, :, columns(lane)].astype(F32)

    def meant_for(lane, s):
        return lax.rem(z + chips - 1 - s, chips) if lane < 2 else lax.rem(z + 1 + s, chips)

    def first(k):
        swap(k).wait_recv()
        for lane in LANES:
            ring[k, lane, 0] = term(k, lane, meant_for(lane, 0)).astype(BF16)
            hop(k, lane, 0).start()

    def middle(k, s):
        for lane in LANES:
            hop(k, lane, s - 1).wait_recv()
            ring[k, lane, s] = (term(k, lane, meant_for(lane, s)) + ring[k, lane, s].astype(F32)).astype(BF16)
            hop(k, lane, s).start()

    def last(k):
        for lane in LANES:
            hop(k, lane, chips - 2).wait_recv()
            g = (term(k, lane, z) + ring[k, lane, chips - 1].astype(F32)).astype(BF16)
            g_ref[k, :, columns(lane)] = g
            squares[...] += g.astype(F32) * g.astype(F32)

    enter([lax.rem(me + o, n) for o in range(1, n)])
    start_load(0)
    squares[...] = jnp.zeros_like(squares)

    @pl.loop(0, tiles)
    def _(index):
        tile(index, swaps=False)

    meet(n - 1)
    swap(jnp.int32(0)).start()

    @pl.loop(0, pairs + 1)
    def _(ii):
        @pl.loop(0, chips - 1)
        def _(s):
            for j in range(2):
                k = 2 * (ii - 1) + j

                @pl.when(jnp.logical_and(ii > 0, jnp.logical_and(s == 0, k > 0)))
                def _():
                    first(k)

                @pl.when(jnp.logical_and(ii > 0, s > 0))
                def _():
                    middle(k, s)

                @pl.when(jnp.logical_and(ii > 1, s == 0))
                def _():
                    last(k - 2)

                if j == 0:

                    @pl.when(jnp.logical_and(ii == 0, s == tiles - 1))
                    def _():
                        first(jnp.int32(0))

                place = 2 * s + j - shift * lax.div(ii, 2)

                @pl.when(jnp.logical_and(ii < pairs, jnp.logical_and(place >= tiles * (1 - lax.div(ii + 2, 3)), place < 2 * tiles)))
                def _():
                    tile(2 * tiles * ii + place)

                if j == 0:

                    @pl.when(jnp.logical_and(ii == 1, s == tiles))
                    def _():
                        for copy in back_states():
                            copy.start()

                if j == 0:
                    due, u = jnp.logical_and(ii == 2, s == late - 1), jnp.int32(backs - 1)
                else:
                    due = jnp.logical_or(jnp.logical_and(ii == 1, s >= tiles), jnp.logical_and(ii == 2, s < late - 1))
                    u = s - tiles + (ii - 1) * (chips - 1)

                @pl.when(due)
                def _():
                    back(u)

    for j in range(2):
        last(jnp.int32(count - 2 + j))

    whole = squares[0:8, 0:128]
    for i in range(r // 8):
        for q in range(quarter // 128):
            if i or q:
                whole = whole + squares[i * 8 : (i + 1) * 8, q * 128 : (q + 1) * 128]
    slots[0] = whole
    sends = [remote(slots.at[0], slots.at[o], all_send.at[o], all_recv.at[o], lax.rem(me + o, n)) for o in range(1, n)]
    for send in sends:
        send.start()
    for send in sends:
        send.wait_recv()
    whole = slots[0]
    for o in range(1, n):
        whole = whole + slots[o]
    total_ref[...] = jnp.full(total_ref.shape, jnp.sum(whole), F32)
    for send in sends:
        send.wait_send()

    @pl.loop(0, count)
    def _(k):
        @pl.loop(0, chips - 1)
        def _(s):
            for lane in LANES:
                hop(k, lane, s).wait_send()

    for j in range(2):
        swap(jnp.int32(count - 2 + j)).wait_send()


SOURCES = ((0, 4, True), (1, 2, False), (1, 3, False), (5, 7, True), (6, 8, False), (6, 9, False))
A0, DY0 = 6, 7


def summed(n, arrays, weights):
    tokens, d = arrays[1].shape[1:]
    ff = arrays[0].shape[2]
    r, chips, count, width = d // n, n // 2, len(SOURCES), ff // 6
    dma = pltpu.SemaphoreType.DMA
    like, any_spec, vmem_spec = jax.ShapeDtypeStruct, pl.BlockSpec(memory_space=ANY), pl.BlockSpec(memory_space=VMEM)
    operands = (*arrays, *weights)
    return pl.pallas_call(
        functools.partial(sum_kernel, n, len(operands)),
        out_shape=(like((count, r, ff), BF16), like((8, 128), F32), like((tokens, ff), BF16), like((tokens, ff), BF16)),
        in_specs=[any_spec] * len(operands),
        out_specs=(vmem_spec, vmem_spec, any_spec, any_spec),
        scratch_shapes=[
            VMEM((2, tokens, d), BF16),
            VMEM((2, tokens, d), BF16),
            VMEM((d, width), BF16),
            VMEM((d, width), BF16),
            VMEM((width, d), BF16),
            VMEM((6, chips, r, ff), BF16),
            VMEM((count, chips, r, ff), BF16),
            VMEM((count, 4, chips, r, ff // 4), BF16),
            VMEM((r, ff // 4), F32),
            VMEM((n, 8, 128), F32),
            dma((2, 2)),
            dma((7,)),
            dma((count,)),
            dma((count,)),
            dma((count, 4, chips - 1)),
            dma((count, 4, chips - 1)),
            dma((n,)),
            dma((n,)),
        ],
        compiler_params=pltpu.CompilerParams(collective_id=0, has_side_effects=True, vmem_limit_bytes=VMEM_BYTES),
        name="gradient_sum",
    )(*operands)


WEIGHTS = ((2, 1), (0, 1), (1, 1), (2, 0), (0, 0), (1, 0))


def pieces(k, array, block):
    name, layer = WEIGHTS[k]
    if name < 2:
        return [(array.at[layer], block)]
    tiles, width = array.shape[-3], array.shape[-1]
    lead = (slice(None),) * (len(array.shape) - 4)
    return [(array.at[(layer, *lead, q)], block.at[(*lead, slice(None), pl.ds(q * width, width))]) for q in range(tiles)]


def own_pieces(k, array, block, me):
    name, layer = WEIGHTS[k]
    if name < 2:
        return [(array.at[layer, me], block)]
    tiles, width = array.shape[-3], array.shape[-1]
    return [(array.at[layer, me, q], block.at[:, pl.ds(q * width, width)]) for q in range(tiles)]


def gather_kernel(n, g_ref, total_ref, *refs):
    w_in, m_in, v_in = (refs[i : i + 3] for i in range(0, 9, 3))
    count, r, ff = g_ref.shape
    w_out = refs[9 : 9 + count]
    m_out, v_out, w_buf, m_buf, v_buf, load_sem, store_sem, ring_send, ring_recv, pair_send, pair_recv = refs[9 + count :]
    half, chunk, chips = ff // 2, ff // 4, n // 2
    me = lax.axis_index("dp")
    z, c = lax.div(me, 2), lax.rem(me, 2)
    partner = 2 * z + 1 - c
    right = 2 * lax.rem(z + 1, chips) + c
    left = 2 * lax.rem(z + chips - 1, chips) + c
    onward = (right, left)

    def loads(k):
        name = WEIGHTS[k][0]
        parts = own_pieces(k, w_in[name], w_buf.at[k], me) + pieces(k, m_in[name], m_buf.at[k]) + pieces(k, v_in[name], v_buf.at[k])
        return [pltpu.make_async_copy(src, dst, load_sem.at[k, i]) for i, (src, dst) in enumerate(parts)]

    def stores(k):
        return (
            pltpu.make_async_copy(w_buf.at[k], w_out[k].at[me], store_sem.at[k, 0]),
            pltpu.make_async_copy(m_buf.at[k], m_out.at[k], store_sem.at[k, 1]),
            pltpu.make_async_copy(v_buf.at[k], v_out.at[k], store_sem.at[k, 2]),
        )

    def came(way, s):
        return lax.rem(z + chips - s, chips) if way == 0 else lax.rem(z + s, chips)

    def part(k, way, s):
        return w_out[k].at[2 * came(way, s) + c, :, pl.ds(way * half, half)]

    def hop(k, way, s, source=None):
        ref = part(k, way, s)
        return remote(ref if source is None else source, ref, ring_send.at[k, way, s], ring_recv.at[k, way, s], onward[way])

    def across(k, way, s, source=None):
        ref = part(k, way, s)
        return remote(ref if source is None else source, ref, pair_send.at[k, way, s], pair_recv.at[k, way, s], partner)

    enter((partner, left, right))
    for k in range(count):
        for copy in loads(k):
            copy.start()
    factor = jnp.minimum(1.0, 0.5 * lax.rsqrt(total_ref[0:1, 0:1] * (1.0 / (count * r * ff * n)) + 1e-30))

    for k in range(count):
        for copy in loads(k):
            copy.wait()

        @pl.loop(0, ff // chunk)
        def _(q):
            cols = pl.ds(pl.multiple_of(q * chunk, chunk), chunk)
            g = g_ref[k, :, cols].astype(F32) * factor
            m = 0.9 * m_buf[k, :, cols] + 0.1 * g
            v = 0.95 * v_buf[k, :, cols] + 0.05 * g * g
            w = w_buf[k, :, cols].astype(F32)
            step = m * lax.rsqrt(v + 1e-8) + 0.1 * w
            m_buf[k, :, cols] = m
            v_buf[k, :, cols] = v
            w_buf[k, :, cols] = (w - 0.02 * step).astype(BF16)

        if k == 0:
            meet(3)
        for way in range(2):
            own = w_buf.at[k, :, pl.ds(way * half, half)]
            hop(k, way, 0, own).start()
            across(k, way, 0, own).start()
        for copy in stores(k):
            copy.start()

    @pl.loop(1, chips)
    def _(s):
        for k in range(count):
            for way in range(2):
                hop(k, way, s - 1).wait_recv()

                @pl.when(s < chips - 1)
                def _():
                    hop(k, way, s).start()

                across(k, way, s).start()

    for k in range(count):
        for copy in stores(k):
            copy.wait()

        @pl.loop(0, chips)
        def _(s):
            for way in range(2):
                across(k, way, s).wait()

                @pl.when(s < chips - 1)
                def _():
                    hop(k, way, s).wait_send()


def stepped(n, g, total, w, m, v):
    count, r, ff = g.shape
    layers, d = w[0].shape[:2]
    chips, tiles = n // 2, ff // d
    dma = pltpu.SemaphoreType.DMA
    any_spec, vmem_spec = pl.BlockSpec(memory_space=ANY), pl.BlockSpec(memory_space=VMEM)
    row = (layers, r, ff), (layers, r, ff), (layers, tiles, r, d)
    whole = (layers, n, r, ff), (layers, n, r, ff), (layers, n, tiles, r, d)
    w = [t.reshape(s) for t, s in zip(w, whole, strict=True)]
    m, v = ([t.reshape(s) for t, s in zip(ts, row, strict=True)] for ts in (m, v))
    m, v = ([pltpu.with_memory_space_constraint(t, HBM) for t in ts] for ts in (m, v))
    held = pl.pallas_call(
        functools.partial(gather_kernel, n),
        out_shape=(*[VMEM((n, r, ff), BF16)] * count, *[jax.ShapeDtypeStruct((count, r, ff), F32)] * 2),
        in_specs=[vmem_spec] * 2 + [any_spec] * 9,
        out_specs=(any_spec,) * (count + 2),
        scratch_shapes=[
            *[VMEM((count, r, ff), t) for t in (BF16, F32, F32)],
            dma((count, 3 * tiles)),
            dma((count, 3)),
            *[dma((count, 2, chips - 1)) for _ in range(2)],
            *[dma((count, 2, chips)) for _ in range(2)],
        ],
        compiler_params=pltpu.CompilerParams(collective_id=1, has_side_effects=True, vmem_limit_bytes=27 * 1024 * 1024),
        name="step_and_gather",
    )(g, total, *w, *m, *v)

    def write_out(*refs):
        w_held, (m_held, v_held, *outs, sem) = refs[:count], refs[count:]
        parts = [
            pair
            for k, (name, _) in enumerate(WEIGHTS)
            for out, block in ((outs[name], w_held[k]), (outs[3 + name], m_held.at[k]), (outs[6 + name], v_held.at[k]))
            for pair in pieces(k, out, block)
        ]
        copies = [pltpu.make_async_copy(block, out, sem.at[i]) for i, (out, block) in enumerate(parts)]
        for copy in copies:
            copy.start()
        for copy in copies:
            copy.wait()

    outs = pl.pallas_call(
        write_out,
        out_shape=tuple(jax.ShapeDtypeStruct(t.shape, t.dtype) for t in (*w, *m, *v)),
        in_specs=[any_spec] * (count + 2),
        out_specs=(any_spec,) * 9,
        scratch_shapes=[dma((3 * count * tiles,))],
        compiler_params=pltpu.CompilerParams(vmem_limit_bytes=1024 * 1024),
        name="write_out",
    )(*held)
    rows = (layers, d, ff), (layers, d, ff), (layers, ff, d)
    blocks = (layers, r, ff), (layers, r, ff), (layers, tiles * r, d)
    return [t.reshape(s) for t, s in zip(outs, (*rows, *blocks, *blocks), strict=True)]


def normed(h):
    wide = h.astype(F32)
    scale = lax.rsqrt(jnp.mean(wide**2, -1, keepdims=True) + 1e-6)
    return (wide * scale).astype(BF16)


def back_through_norm(h, da):
    wide, g = h.astype(F32), da.astype(F32)
    mean = jnp.mean(wide**2, -1, keepdims=True) + 1e-6
    scale = lax.rsqrt(mean)
    inner = jnp.mean(g * wide, -1, keepdims=True)
    return (scale * g - wide * (inner * scale / mean)).astype(BF16)


def back_through_product(gate, up, s, dhid):
    p = dhid.astype(BF16).astype(F32)
    return (p * up * (s * (1 + gate * (1 - s)))).astype(BF16), (p * (gate * s)).astype(BF16)


def dot(a, b):
    return jnp.dot(a, b, preferred_element_type=F32)


def dot_t(a, b):
    return lax.dot_general(a, b, (((1,), (1,)), ((), ())), preferred_element_type=F32)


def layers_kernel(chunks, x_ref, dy_ref, wg_ref, wu_ref, wd_ref, a_ref, hid_ref, dgate_ref, dup_ref, dh_ref, h, acc_g, acc_u):
    turn, i, end = pl.program_id(0) == 1, pl.program_id(1), pl.num_programs(1) - 1
    first = jnp.logical_not(turn)
    size = x_ref.shape[0] // chunks

    @pl.when(jnp.logical_and(first, i == 0))
    def _():
        a_ref[...] = normed(x_ref[...])
        acc_g[...] = jnp.zeros_like(acc_g)

    @pl.when(jnp.logical_and(turn, i == 0))
    def _():
        a_ref[...] = normed(h[...])
        acc_g[...] = jnp.zeros_like(acc_g)
        acc_u[...] = jnp.zeros_like(acc_u)

    @pl.when(first)
    def _():
        for q in range(chunks):
            rows = slice(q * size, (q + 1) * size)
            gate, up = dot(a_ref[rows], wg_ref[...]), dot(a_ref[rows], wu_ref[...])
            hid = (gate * jax.nn.sigmoid(gate) * up).astype(BF16)
            hid_ref[rows] = hid
            acc_g[rows] += dot(hid, wd_ref[...])

    @pl.when(turn)
    def _():
        for q in range(chunks):
            rows = slice(q * size, (q + 1) * size)
            gate, up = dot(a_ref[rows], wg_ref[...]), dot(a_ref[rows], wu_ref[...])
            dhid = dot_t(dy_ref[rows], wd_ref[...])
            s = jax.nn.sigmoid(gate)
            hid_ref[rows] = (gate * s * up).astype(BF16)
            dgate, dup = back_through_product(gate, up, s, dhid)
            dgate_ref[rows], dup_ref[rows] = dgate, dup
            acc_g[rows] += dot_t(dgate, wg_ref[...])
            acc_u[rows] += dot_t(dup, wu_ref[...])

    @pl.when(jnp.logical_and(first, i == end))
    def _():
        h[...] = x_ref[...] + acc_g[...].astype(BF16)

    @pl.when(jnp.logical_and(turn, i == end))
    def _():
        da = acc_g[...].astype(BF16) + acc_u[...].astype(BF16)
        dh_ref[...] = dy_ref[...] + back_through_norm(h[...], da)


def operands(x, dy, w_gate, w_up, w_down):
    (tokens, d), (layers, _, ff) = x.shape, w_gate.shape
    tile, chunks = ff // 6, 2
    like = jax.ShapeDtypeStruct
    state = pl.BlockSpec((tokens, d), lambda l, i: (0, 0))
    into = pl.BlockSpec((None, d, tile), lambda l, i: (l, 0, i))
    last = pl.BlockSpec((tokens, tile), lambda l, i: (0, l * i))
    a, hid, dgate, dup, dh = pl.pallas_call(
        functools.partial(layers_kernel, chunks),
        grid=(layers, ff // tile),
        out_shape=(
            like((layers, tokens, d), BF16),
            like((layers, tokens, ff), BF16),
            like((tokens, ff), BF16),
            like((tokens, ff), BF16),
            like((tokens, d), BF16),
        ),
        in_specs=[state, state, into, into, pl.BlockSpec((None, tile, d), lambda l, i: (l, i, 0))],
        out_specs=(
            pl.BlockSpec((None, tokens, d), lambda l, i: (l, 0, 0)),
            pl.BlockSpec((None, tokens, tile), lambda l, i: (l, 0, i)),
            last,
            last,
            state,
        ),
        scratch_shapes=[VMEM((tokens, d), BF16), VMEM((tokens, d), F32), VMEM((tokens, d), F32)],
        compiler_params=pltpu.CompilerParams(vmem_limit_bytes=58 * 1024 * 1024, dimension_semantics=("arbitrary", "arbitrary")),
        name="layers",
    )(x, dy, w_gate, w_up, w_down)
    return hid, a, dgate, dup, dy, dh


def solution(mesh):
    n = mesh.shape["dp"]

    def device(x, dy, *arrays):
        w, m, v = (arrays[i : i + 3] for i in (0, 3, 6))
        g, total, *_ = summed(n, operands(x[0], dy[0], *w), w)
        return tuple(stepped(n, g, total, w, m, v))

    whole, rows = P(None, None, None), P(None, "dp", None)
    tokens = P(("rep", "dp"), None, None)
    return jax.shard_map(
        device,
        mesh=mesh,
        in_specs=(tokens, tokens, *[whole] * 3, *[rows] * 6),
        out_specs=(*[P("rep", None, None)] * 3, *[P("rep", "dp", None)] * 6),
        check_vma=False,
    )
```
